32 devices in a mesh: wide: 8 (over y, x, core), narrow: 4 (over z).
Axes of the slice: x: 2, y: 2, z: 4, core: 2. Of those that a mesh axis runs over, the one named last changes fastest.
Arguments:
- node_features: bfloat16 [2048, 25, 128], P(('wide', 'narrow')), may hold values from -6 to 6
- frames: bfloat16 [2048, 48, 165], P(('wide', 'narrow')), may hold values from -6 to 6
- radial: bfloat16 [2048, 48, 128], P(('wide', 'narrow')), may hold values from 0.29882812 to 3
- neighbours: int32 [2048, 48], P(('wide', 'narrow')), may hold values from 0 to 2047, as said below
- counts: int32 [2048], P(('wide', 'narrow')), may hold values from 16 to 48
- coefficients: float32 [32], P('wide'), may hold values from 0.05 to 0.5
- w_zero: bfloat16 [32, 640, 640], P('wide'), may hold values from -0.25 to 0.25
- w_one: bfloat16 [32, 2, 512, 512], P('wide'), may hold values from -0.1875 to 0.1875
- w_two: bfloat16 [32, 2, 384, 384], P('wide'), may hold values from -0.21875 to 0.21875
- w_three: bfloat16 [32, 2, 256, 256], P('wide'), may hold values from -0.25 to 0.25
- w_four: bfloat16 [32, 2, 128, 128], P('wide'), may hold values from -0.375 to 0.375
Outputs:
- conv_out: float32 [2048, 25, 128], P(('wide', 'narrow'))
The draws below stay inside these ranges and needn't reach their ends.
Inputs may be any that keep to these rules, and one draw needn't show every extreme that they name: `neighbours`: each neighbour of an atom lies in the atom's own aligned block of 64 atoms or in one of the two cyclically adjacent blocks. `counts`: slots at or beyond an atom's count are padding and carry arbitrary indices.
All inputs are finite; a program needn't handle non-finite values.
Results may differ from the reference program's by a relative error of at most 0.02.
Values may be sent and summed in bfloat16 or wider, within the bound.
A program may use at most 192 MiB of HBM per device.

```python
import math
import jax
import jax.numpy as jnp
from jax import lax

C = 128
EXPERTS = 32
NEIGH = 48
ATOM_DEV = 64
ATOMS = 2048
N_WIDE = 8


def draw_neighbours(key, part):
    block_count = ATOMS // ATOM_DEV
    side_key, position_key = jax.random.split(jax.random.fold_in(key, 11))
    home_block = (jnp.arange(ATOMS, dtype=jnp.int32) // ATOM_DEV)[:, None]
    offset_step = jax.random.randint(side_key, (ATOMS, NEIGH), -1, 2)
    position = jax.random.randint(position_key, (ATOMS, NEIGH), 0, ATOM_DEV)
    return ((home_block + offset_step + block_count) % block_count * ATOM_DEV + position).astype(jnp.int32)


def with_ends(values, rng, low, high):
    dims = values.shape
    index_at = [jax.random.randint(jax.random.fold_in(rng, axis), (), 0, dims[axis]) for axis in range(len(dims))]
    values = values.at[tuple(index_at)].set(low)
    longest = dims.index(max(dims))
    index_at[longest] = (index_at[longest] + 1) % dims[longest]
    return values.at[tuple(index_at)].set(high)


def block_levels(own_key, shape, cuts, least, top_value):
    factor_of = 1.0
    for dim, parts in cuts:
        steps = jax.random.uniform(jax.random.fold_in(jax.random.fold_in(own_key, 6), dim), (parts,), jnp.float32, least / len(cuts), top_value / len(cuts))
        factor_of = factor_of * jnp.repeat(jnp.exp(steps), shape[dim] // parts).reshape((-1,) + (1,) * (len(shape) - 1 - dim))
    return factor_of


def noise(own_key, dims, spread, most, cuts=(), kind=jnp.bfloat16):
    factor_of = block_levels(own_key, dims, cuts, -0.22, 0.18) if cuts else 1.0
    array = jax.random.normal(own_key, dims, jnp.float32) * spread * factor_of
    return jnp.minimum(jnp.maximum(array, -most), most).astype(kind)


def setup_inputs(seed: int = 0) -> dict:
    key_list = jax.random.split(jax.random.key(seed), 12)
    return {
        "node_features": noise(key_list[0], (ATOMS, 25, C), 1.0, 6.0, ((0, 32),)),
        "frames": noise(key_list[1], (ATOMS, NEIGH, 165), 0.45, 6.0, ((0, 32),)),
        "radial": jnp.clip(jnp.exp(math.log(3.0) - 2.306499 * jax.random.uniform(key_list[2], (ATOMS, NEIGH, C), jnp.float32) ** block_levels(key_list[2], (ATOMS, NEIGH, C), ((0, 32),), -0.2, 0.2)), 0.29882812, 3.0).astype(jnp.bfloat16),
        "neighbours": draw_neighbours(jax.random.fold_in(key_list[11], 71), 0),
        "counts": with_ends(jax.random.randint(key_list[4], (ATOMS,), NEIGH // 3, NEIGH + 1), jax.random.fold_in(key_list[4], 1), NEIGH // 3, NEIGH).astype(jnp.int32),
        "coefficients": jnp.clip(jnp.exp(math.log(0.5) - 2.3025851 * jax.random.uniform(key_list[5], (EXPERTS,), jnp.float32) ** block_levels(key_list[5], (EXPERTS,), ((0, 8),), -0.2, 0.2)), 0.05, 0.5),
        "w_zero": noise(key_list[6], (EXPERTS, 5 * C, 5 * C), (5 * C) ** -0.5, 0.25, ((0, 8),)),
        "w_one": noise(key_list[7], (EXPERTS, 2, 4 * C, 4 * C), (8 * C) ** -0.5, 0.1875, ((0, 8),)),
        "w_two": noise(key_list[8], (EXPERTS, 2, 3 * C, 3 * C), (6 * C) ** -0.5, 0.21875, ((0, 8),)),
        "w_three": noise(key_list[9], (EXPERTS, 2, 2 * C, 2 * C), (4 * C) ** -0.5, 0.25, ((0, 8),)),
        "w_four": noise(key_list[10], (EXPERTS, 2, C, C), (2 * C) ** -0.5, 0.375, ((0, 8),)),
    }


def rotate(frames, features, inverse):
    pieces = []
    offset = 0
    for degree in range(5):
        order_size = 2 * degree + 1
        frame_block = frames[:, offset:offset + order_size * order_size].reshape(-1, order_size, order_size).astype(jnp.float32)
        component = features[:, degree * degree:degree * degree + order_size, :].astype(jnp.float32)
        if inverse:
            pieces.append(jnp.einsum('rji,rjc->ric', frame_block, component, precision=lax.Precision.HIGHEST))
        else:
            pieces.append(jnp.einsum('rij,rjc->ric', frame_block, component, precision=lax.Precision.HIGHEST))
        offset += order_size * order_size
    return jnp.concatenate(pieces, axis=1)

def convolve(rotated, merged):
    row_count = rotated.shape[0]
    channels = rotated.shape[2]
    outputs = [None] * 25
    central = jnp.stack([rotated[:, degree * degree + degree] for degree in range(5)], axis=1).reshape(row_count, 5 * channels)
    result = jnp.dot(central, merged[0], preferred_element_type=jnp.float32).reshape(row_count, 5, channels)
    for degree in range(5):
        outputs[degree * degree + degree] = result[:, degree]
    for order in range(1, 5):
        kept = 5 - order
        plus = jnp.stack([rotated[:, degree * degree + degree + order] for degree in range(order, 5)], axis=1).reshape(row_count, kept * channels)
        minus = jnp.stack([rotated[:, degree * degree + degree - order] for degree in range(order, 5)], axis=1).reshape(row_count, kept * channels)
        stacked = jnp.concatenate([plus, minus], axis=0)
        weight_pair = merged[order]
        real_part = jnp.dot(stacked, weight_pair[0], preferred_element_type=jnp.float32)
        imag_part = jnp.dot(stacked, weight_pair[1], preferred_element_type=jnp.float32)
        out_plus = (real_part[:row_count] - imag_part[row_count:]).reshape(row_count, kept, channels)
        out_minus = (real_part[row_count:] + imag_part[:row_count]).reshape(row_count, kept, channels)
        for column, degree in enumerate(range(order, 5)):
            outputs[degree * degree + degree + order] = out_plus[:, column]
            outputs[degree * degree + degree - order] = out_minus[:, column]
    return jnp.stack(outputs, axis=1)

def messages(gathered, frames, radial, merged):
    rotated = (rotate(frames, gathered, False) * radial.astype(jnp.float32)[:, None, :]).astype(jnp.bfloat16)
    mixed = convolve(rotated, merged)
    scalar = mixed[:, 0:1, :]
    gated = jnp.concatenate([jax.nn.silu(scalar), mixed[:, 1:, :] * jax.nn.sigmoid(scalar)], axis=1)
    return rotate(frames, gated, True)

def merge_weights(coefficients, weights):
    grouped_coeff = coefficients.reshape(N_WIDE, -1)
    grouped = weights.astype(jnp.float32).reshape((N_WIDE, grouped_coeff.shape[1]) + weights.shape[1:])
    partials = jnp.einsum('ge,ge...->g...', grouped_coeff, grouped, precision=lax.Precision.HIGHEST).astype(jnp.bfloat16)
    partials = lax.optimization_barrier(partials)
    return lax.optimization_barrier(jnp.sum(partials.astype(jnp.float32), axis=0)).astype(jnp.bfloat16)

def reference(node_features, frames, radial, neighbours, counts, coefficients, w_zero, w_one, w_two, w_three, w_four):
    merged = tuple((merge_weights(coefficients, weights) for weights in (w_zero, w_one, w_two, w_three, w_four)))
    atoms_total = node_features.shape[0]
    channels = node_features.shape[2]
    block_count = atoms_total // ATOM_DEV
    live_slots = (lax.broadcasted_iota(jnp.int32, neighbours.shape, 1) < counts[:, None]).astype(jnp.float32)

    def one_block(inputs):
        index_block, frame_block, radial_block, live_block = inputs
        gathered = jnp.take(node_features, index_block.reshape(-1), axis=0)
        result = messages(gathered, frame_block.reshape(-1, 165), radial_block.reshape(-1, channels), merged)
        result = result.reshape(ATOM_DEV, NEIGH, 25, channels)
        return lax.optimization_barrier(jnp.sum(result * live_block[:, :, None, None], axis=1))
    summed = lax.map(one_block, (neighbours.reshape(block_count, ATOM_DEV, NEIGH), frames.reshape(block_count, ATOM_DEV, NEIGH, 165), radial.reshape(block_count, ATOM_DEV, NEIGH, channels), live_slots.reshape(block_count, ATOM_DEV, NEIGH)))
    summed = summed.reshape(atoms_total, 25, channels)
    return summed / jnp.sqrt(counts.astype(jnp.float32))[:, None, None]
```

```python
import functools

import jax
import jax.numpy as jnp
import numpy as np
from jax import lax
from jax.experimental import pallas as pl
from jax.experimental.pallas import tpu as pltpu
from jax.sharding import PartitionSpec as P

DEGREES = 5
COMPONENTS = DEGREES * DEGREES
AXES = ("wide", "narrow")
MESH = pl.DeviceIdType.MESH


def flat_rows(weights):
    return weights.reshape(weights.shape[0], -1, weights.shape[-1])


def remote(src, dst, send, recv, device):
    return pltpu.make_async_remote_copy(
        src_ref=src,
        dst_ref=dst,
        send_sem=send,
        recv_sem=recv,
        device_id=device,
        device_id_type=MESH,
    )


def exchange_kernel(sizes, coefficient_ref, features_ref, *refs):
    wide, narrow, count = sizes
    stacks = refs[:count]
    sides_ref, merged_ref = refs[count : count + 2]
    staged = refs[count + 2 : 2 * count + 2]
    (
        partial_ref,
        received_ref,
        share_ref,
        load_sem,
        halo_send,
        halo_recv,
        send_sem,
        recv_sem,
        line_send,
        line_recv,
        plane_send,
        plane_recv,
        pair_send,
        pair_recv,
        local_sem,
    ) = refs[2 * count + 2 :]
    my_wide = lax.axis_index("wide")
    my_narrow = lax.axis_index("narrow")
    part = partial_ref.shape[0] // wide
    chips = wide // 2
    my_chip = my_wide // 2
    my_core = lax.rem(my_wide, 2)

    loads = []
    for at, (stack, stage) in enumerate(zip(stacks, staged)):
        rows = stage.shape[1]
        loads.append(
            pltpu.make_async_copy(
                stack.at[:, pl.ds(pl.multiple_of(my_narrow * rows, 16), rows), :],
                stage,
                load_sem.at[at],
            )
        )
        loads[-1].start()

    total = wide * narrow
    me = my_wide * narrow + my_narrow
    after = lax.rem(me + 1, total)
    before = lax.rem(me + total - 1, total)
    place = lambda flat: (flat // narrow, lax.rem(flat, narrow))
    peers = [(lax.rem(my_wide + hop, wide), my_narrow) for hop in range(1, wide)]
    line = [(my_wide, lax.rem(my_narrow + hop, narrow)) for hop in range(1, narrow)]
    greeted = [place(after), place(before)] + peers + line
    barrier = pltpu.get_barrier_semaphore()
    for device in greeted:
        pl.semaphore_signal(barrier, inc=1, device_id=device, device_id_type=MESH)
    pl.semaphore_wait(barrier, len(greeted))

    halo = []
    for side, device in enumerate([place(after), place(before)]):
        halo.append(
            remote(
                features_ref, sides_ref.at[side], halo_send.at[side], halo_recv.at[side], device
            )
        )
        halo[-1].start()

    offset = 0
    for load, stage in zip(loads, staged):
        load.wait()
        experts, rows, columns = stage.shape
        for block in range(columns // 128):
            lanes = pl.ds(block * 128, 128)
            value = coefficient_ref[0] * stage[0, :, lanes].astype(jnp.float32)
            for expert in range(1, experts):
                value = value + coefficient_ref[expert] * stage[expert, :, lanes].astype(
                    jnp.float32
                )
            partial_ref[pl.ds(offset, rows), :] = value.astype(jnp.bfloat16)
            offset += rows
    if offset < partial_ref.shape[0]:
        rest = partial_ref.shape[0] - offset
        partial_ref[pl.ds(offset, rest), :] = jnp.zeros((rest, 128), jnp.bfloat16)

    scatter = []
    for hop, device in enumerate(peers):
        target = device[0]
        scatter.append(
            remote(
                partial_ref.at[pl.ds(pl.multiple_of(target * part, 16), part), :],
                received_ref.at[hop],
                send_sem.at[hop],
                recv_sem.at[hop],
                device,
            )
        )
        scatter[-1].start()
    summed = partial_ref[pl.ds(pl.multiple_of(my_wide * part, 16), part), :].astype(jnp.float32)
    for hop in range(wide - 1):
        scatter[hop].wait_recv()
        summed = summed + received_ref[hop].astype(jnp.float32)
    share_ref[...] = summed.astype(jnp.bfloat16)

    keep = pltpu.make_async_copy(share_ref, merged_ref.at[my_narrow, my_wide], local_sem)
    keep.start()
    partner = (my_wide + 1 - 2 * my_core, my_narrow)
    along = []
    for hop in range(1, narrow):
        along.append(
            remote(
                share_ref,
                merged_ref.at[my_narrow, my_wide],
                line_send.at[hop - 1],
                line_recv.at[hop - 1],
                line[hop - 1],
            )
        )
        along[-1].start()
    across = []
    paired = []

    def forward(hop):
        origin = lax.rem(my_narrow + narrow - hop, narrow)
        slot = merged_ref.at[origin, my_wide]
        source = share_ref if hop == 0 else slot
        for step in range(1, chips):
            at = hop * (chips - 1) + step - 1
            target = lax.rem(my_chip + step, chips) * 2 + my_core
            across.append(
                remote(source, slot, plane_send.at[at], plane_recv.at[at], (target, my_narrow))
            )
            across[-1].start()
        at = hop * chips
        paired.append(remote(source, slot, pair_send.at[at], pair_recv.at[at], partner))
        paired[-1].start()

    def relay(hop):
        origin = lax.rem(my_narrow + narrow - hop, narrow)
        for step in range(1, chips):
            across[hop * (chips - 1) + step - 1].wait_recv()
            owner = lax.rem(my_chip + chips - step, chips) * 2 + my_core
            slot = merged_ref.at[origin, owner]
            at = hop * chips + step
            paired.append(remote(slot, slot, pair_send.at[at], pair_recv.at[at], partner))
            paired[-1].start()

    forward(0)
    for hop in range(1, narrow):
        along[hop - 1].wait_recv()
        forward(hop)
    for hop in range(narrow):
        relay(hop)
    for copy in paired:
        copy.wait_recv()
    for copy in scatter + along + across + paired:
        copy.wait_send()
    keep.wait()
    for copy in halo:
        copy.wait()


def exchange(features, coefficients, stacks):
    wide = lax.axis_size("wide")
    narrow = lax.axis_size("narrow")
    stacks = [flat_rows(w) for w in stacks]
    staged = [(w.shape[0], w.shape[1] // narrow, w.shape[2]) for w in stacks]
    rows = sum(shape[1] * shape[2] // 128 for shape in staged)
    unit = 16 * wide
    rows = -(-rows // unit) * unit
    part = rows // wide
    chips = wide // 2
    anywhere = pl.BlockSpec(memory_space=pl.ANY)
    dma = lambda n: pltpu.SemaphoreType.DMA((n,))
    return pl.pallas_call(
        functools.partial(exchange_kernel, (wide, narrow, len(stacks))),
        in_specs=[pl.BlockSpec(memory_space=pltpu.SMEM)] + [anywhere] * (1 + len(stacks)),
        out_specs=[anywhere, anywhere],
        out_shape=[
            jax.ShapeDtypeStruct((2,) + features.shape, features.dtype),
            jax.ShapeDtypeStruct((narrow, wide, part, 128), jnp.bfloat16),
        ],
        scratch_shapes=[pltpu.VMEM(shape, jnp.bfloat16) for shape in staged]
        + [
            pltpu.VMEM((rows, 128), jnp.bfloat16),
            pltpu.VMEM((wide - 1, part, 128), jnp.bfloat16),
            pltpu.VMEM((part, 128), jnp.bfloat16),
            dma(len(stacks)),
            dma(2),
            dma(2),
            dma(wide - 1),
            dma(wide - 1),
            dma(narrow - 1),
            dma(narrow - 1),
            dma(narrow * (chips - 1)),
            dma(narrow * (chips - 1)),
            dma(narrow * chips),
            dma(narrow * chips),
            pltpu.SemaphoreType.DMA,
        ],
        compiler_params=pltpu.CompilerParams(collective_id=0, has_side_effects=True),
    )(coefficients, features, *stacks)


def order_starts():
    starts = []
    start = 0
    for order in range(DEGREES):
        starts.append(start)
        start += (DEGREES - order) * (1 if order == 0 else 2)
    return starts


def turn(xs, frame_ref, radial, turned_ref, tile):
    starts = order_starts()
    offset = 0
    for degree in range(DEGREES):
        size = 2 * degree + 1
        base = degree * degree
        for p in range(size):
            value = frame_ref[offset + p * size] * xs(base)
            for q in range(1, size):
                value = value + frame_ref[offset + p * size + q] * xs(base + q)
            order = abs(p - degree)
            at = starts[order] + degree - order
            if p < degree:
                at += DEGREES - order
            turned_ref[tile(at), :] = value * radial
        offset += size * size


def convolve_kernel(
    shapes,
    slots,
    neighbours_ref,
    counts_ref,
    frames_ref,
    radial_ref,
    features_ref,
    sides_ref,
    merged_ref,
    out_ref,
    extended_ref,
    rows_ref,
    source_ref,
    frame_ref,
    spread_ref,
    radial_t_ref,
    turned_ref,
    gated_ref,
    total_ref,
    column_ref,
    *weight_refs,
):
    step = pl.program_id(0)
    components, atoms, channels = out_ref.shape
    lanes, entries = frames_ref.shape
    members = merged_ref.shape[0]
    starts = order_starts()
    iota = lambda shape, axis: lax.broadcasted_iota(jnp.int32, shape, axis)

    @pl.when(step == 0)
    def _():
        total_ref[...] = jnp.zeros_like(total_ref)
        for component in range(components):
            stacked = jnp.concatenate(
                [sides_ref[0, component], features_ref[component], sides_ref[1, component]], axis=0
            )
            extended_ref[pl.ds(component * channels, channels), :] = jnp.transpose(stacked)
        wide, narrow = lax.axis_size("wide"), lax.axis_size("narrow")
        start = (lax.axis_index("wide") * narrow + lax.axis_index("narrow")) * atoms
        everything = atoms * wide * narrow
        relative = neighbours_ref[...] - (start - atoms)
        relative = jnp.where(relative < 0, relative + everything, relative)
        relative = jnp.where(relative >= everything, relative - everything, relative)
        relative = jnp.minimum(relative, 255)
        rows_ref[...] = relative.astype(jnp.float32).astype(jnp.bfloat16)
        square = (atoms, atoms)
        diagonal = iota(square, 0) == iota(square, 1)
        count = jnp.sum(
            jnp.where(diagonal, counts_ref[...].astype(jnp.float32), 0.0), axis=1, keepdims=True
        )
        column_ref[...] = jnp.broadcast_to(count, column_ref.shape)
        offset = 0
        for weight_ref, (rows, columns) in zip(weight_refs, shapes):
            part = rows // members
            for block in range(columns // 128):
                whole = jnp.concatenate(
                    [merged_ref[m, pl.ds(offset, part), :] for m in range(members)], axis=0
                )
                weight_ref[pl.ds(block * 128, 128), :] = jnp.transpose(whole)
                offset += part

    edge = iota((1, lanes), 1) + step * lanes
    home = edge // slots
    slot = edge - home * slots

    chosen = (iota((atoms, lanes), 0) == home).astype(jnp.bfloat16)
    spread = jnp.dot(rows_ref[...], chosen, preferred_element_type=jnp.float32)
    index = jnp.sum(
        jnp.where(iota((slots, lanes), 0) == slot, spread, 0.0), axis=0, keepdims=True
    ).astype(jnp.int32)
    extended = extended_ref.shape[1]
    picked = (iota((extended, lanes), 0) == index).astype(jnp.bfloat16)
    for component in range(components):
        block = pl.ds(component * channels, channels)
        source_ref[block, :] = jnp.dot(
            extended_ref[block, :], picked, preferred_element_type=jnp.float32
        ).astype(jnp.bfloat16)

    padded = frame_ref.shape[0]
    eye = (iota((padded, entries), 0) == iota((padded, entries), 1)).astype(jnp.bfloat16)
    across = (((1,), (1,)), ((), ()))
    frame_ref[...] = lax.dot_general(
        eye, frames_ref[...], across, preferred_element_type=jnp.float32
    )
    eye = (iota((channels, channels), 0) == iota((channels, channels), 1)).astype(jnp.bfloat16)
    radial_t_ref[...] = lax.dot_general(
        eye, radial_ref[...], across, preferred_element_type=jnp.float32
    ).astype(jnp.bfloat16)
    for k in range(entries):
        row = frame_ref[pl.ds(k, 1), :]
        spread_ref[k] = jnp.broadcast_to(row, spread_ref.shape[1:]).astype(jnp.bfloat16)

    height = spread_ref.shape[1]

    def rotate(i, carried):
        row = pl.multiple_of(i * height, height)
        tile = lambda place: pl.ds(pl.multiple_of(place * channels + row, height), height)
        turn(
            lambda q: source_ref[tile(q), :],
            spread_ref,
            radial_t_ref[pl.ds(row, height), :],
            turned_ref,
            tile,
        )
        return carried

    lax.fori_loop(0, channels // height, rotate, 0)

    central = jnp.dot(
        weight_refs[0][...],
        turned_ref[pl.ds(0, DEGREES * channels), :],
        preferred_element_type=jnp.float32,
    )
    gate = 1.0 / (1.0 + jnp.exp(-central[:channels]))
    for degree in range(DEGREES):
        gated_ref[pl.ds((degree * degree + degree) * channels, channels), :] = (
            central[degree * channels : (degree + 1) * channels] * gate
        ).astype(jnp.bfloat16)
    for order in range(1, DEGREES):
        kept = DEGREES - order
        tall = kept * channels
        plus = turned_ref[pl.ds(starts[order] * channels, tall), :]
        minus = turned_ref[pl.ds(starts[order] * channels + tall, tall), :]
        for side in range(2):
            pair = [plus, -minus] if side == 0 else [minus, plus]
            mixed = jnp.dot(
                weight_refs[order][...],
                jnp.concatenate(pair, axis=0),
                preferred_element_type=jnp.float32,
            )
            for column in range(kept):
                degree = order + column
                component = degree * degree + degree + (order if side == 0 else -order)
                gated_ref[pl.ds(component * channels, channels), :] = (
                    mixed[column * channels : (column + 1) * channels] * gate
                ).astype(jnp.bfloat16)

    window = 8
    first = jnp.minimum((step * lanes) // slots, atoms - window)
    position = slot + slots * (home - first) - slots * iota((window, lanes), 0)
    count = column_ref[pl.ds(first, window), :]
    count = jnp.concatenate([count] * (lanes // channels), axis=1)
    live = jnp.where(
        (position >= 0) & (position.astype(jnp.float32) < count) & (position < slots), 1.0, 0.0
    )
    offset = 0
    for degree in range(DEGREES):
        size = 2 * degree + 1
        summed = None
        for q in range(size):
            left = jnp.concatenate(
                [
                    jnp.broadcast_to(frame_ref[pl.ds(offset + q * size + p, 1), :], live.shape) * live
                    for p in range(size)
                ],
                axis=0,
            ).astype(jnp.bfloat16)
            block = pl.ds((degree * degree + q) * channels, channels)
            term = lax.dot_general(
                left, gated_ref[block, :], across, preferred_element_type=jnp.float32
            )
            summed = term if summed is None else summed + term
        for p in range(size):
            at = degree * degree + p
            total_ref[at, pl.ds(first, window), :] = (
                total_ref[at, pl.ds(first, window), :] + summed[p * window : (p + 1) * window]
            )
        offset += size * size

    @pl.when(step == pl.num_programs(0) - 1)
    def _():
        scale = 1.0 / jnp.sqrt(column_ref[...])
        for component in range(components):
            out_ref[component] = total_ref[component] * scale


def body(
    node_features,
    frames,
    radial,
    neighbours,
    counts,
    coefficients,
    w_zero,
    w_one,
    w_two,
    w_three,
    w_four,
):
    atoms, components, channels = node_features.shape
    slots = neighbours.shape[1]
    entries = frames.shape[2]
    edges = atoms * slots
    stacks = (w_zero, w_one, w_two, w_three, w_four)
    features = node_features.transpose(1, 0, 2)
    sides, merged = exchange(features, coefficients, stacks)
    merged = merged.reshape(merged.shape[0], -1, 128)
    shapes = [(int(np.prod(w.shape[1:-1])), w.shape[-1]) for w in stacks]

    lanes = 256
    height = 16
    padded = -(-entries // 16) * 16
    whole = lambda shape: pl.BlockSpec(shape, lambda i: (0,) * len(shape))
    rows = lambda width: pl.BlockSpec((lanes, width), lambda i: (i, 0))
    out = pl.pallas_call(
        functools.partial(convolve_kernel, shapes, slots),
        grid=(edges // lanes,),
        in_specs=[
            whole((slots, atoms)),
            whole((1, atoms)),
            rows(entries),
            rows(channels),
            whole(features.shape),
            whole(sides.shape),
            whole(merged.shape),
        ],
        out_specs=whole((components, atoms, channels)),
        out_shape=jax.ShapeDtypeStruct((components, atoms, channels), jnp.float32),
        scratch_shapes=[
            pltpu.VMEM((components * channels, 3 * atoms), jnp.bfloat16),
            pltpu.VMEM((slots, atoms), jnp.bfloat16),
            pltpu.VMEM((components * channels, lanes), jnp.bfloat16),
            pltpu.VMEM((padded, lanes), jnp.float32),
            pltpu.VMEM((entries, height, lanes), jnp.bfloat16),
            pltpu.VMEM((channels, lanes), jnp.bfloat16),
            pltpu.VMEM((components * channels, lanes), jnp.bfloat16),
            pltpu.VMEM((components * channels, lanes), jnp.bfloat16),
            pltpu.VMEM((components, atoms, channels), jnp.float32),
            pltpu.VMEM((atoms, channels), jnp.float32),
        ]
        + [pltpu.VMEM((n, k), jnp.bfloat16) for k, n in shapes],
        compiler_params=pltpu.CompilerParams(
            dimension_semantics=("arbitrary",), vmem_limit_bytes=56 * 1024 * 1024
        ),
    )(
        neighbours.T,
        counts.reshape(1, atoms),
        frames.reshape(edges, entries),
        radial.reshape(edges, channels),
        features,
        sides,
        merged,
    )
    return out.transpose(1, 0, 2)


def solution(mesh):
    spread = lambda rest: P(AXES, *([None] * rest))
    in_specs = (
        spread(2),
        spread(2),
        spread(2),
        spread(1),
        spread(0),
        P("wide"),
        P("wide", None, None),
        P("wide", None, None, None),
        P("wide", None, None, None),
        P("wide", None, None, None),
        P("wide", None, None, None),
    )
    return jax.shard_map(body, mesh=mesh, in_specs=in_specs, out_specs=spread(2), check_vma=False)
```

```python
import functools

import jax
import jax.numpy as jnp
import numpy as np
from jax import lax
from jax.experimental import pallas as pl
from jax.experimental.pallas import tpu as pltpu
from jax.sharding import PartitionSpec as P

DEGREES = 5
COMPONENTS = DEGREES * DEGREES
AXES = ("wide", "narrow")
MESH = pl.DeviceIdType.MESH
PLAN = (2, 5, 8, 10, 13, 18, 23)


def flat_rows(weights):
    return weights.reshape(weights.shape[0], -1, weights.shape[-1])


def remote(src, dst, send, recv, device):
    return pltpu.make_async_remote_copy(
        src_ref=src,
        dst_ref=dst,
        send_sem=send,
        recv_sem=recv,
        device_id=device,
        device_id_type=MESH,
    )


def spans():
    return [(degree, degree * degree, 2 * degree + 1) for degree in reversed(range(DEGREES))]


def iota(shape, axis):
    return lax.broadcasted_iota(jnp.int32, shape, axis)


def eye(rows, columns):
    return (iota((rows, columns), 0) == iota((rows, columns), 1)).astype(jnp.bfloat16)


ACROSS = (((1,), (1,)), ((), ()))


def exchange_kernel(sizes, plan, coefficient_ref, neighbours_ref, *refs):
    wide, narrow, count = sizes
    features_ref, frames_ref, radial_ref = refs[:3]
    refs = refs[3:]
    stacks = refs[:count]
    turned_ref, merged_ref = refs[count : count + 2]
    staged = refs[count + 2 : 2 * count + 2]
    (
        partial_ref,
        received_ref,
        share_ref,
        extended_ref,
        upright_ref,
        frames_v,
        radial_v,
        rows_ref,
        picked_ref,
        frame_t,
        radial_t,
        source_ref,
        spread_ref,
        kept_ref,
        load_sem,
        own_sem,
        halo_send,
        halo_recv,
        send_sem,
        recv_sem,
        line_send,
        line_recv,
        plane_send,
        plane_recv,
        pair_send,
        pair_recv,
        local_sem,
        turned_sem,
    ) = refs[2 * count + 2 :]
    my_wide = lax.axis_index("wide")
    my_narrow = lax.axis_index("narrow")
    part = partial_ref.shape[0] // wide
    chips = wide // 2
    my_chip = my_wide // 2
    my_core = lax.rem(my_wide, 2)
    slots, atoms = neighbours_ref.shape
    blocks, _, lanes = picked_ref.shape
    entries = frames_v.shape[1]
    channels = radial_v.shape[1]
    extended = extended_ref.shape[1]

    loads = []
    for at, (stack, stage) in enumerate(zip(stacks, staged)):
        rows = stage.shape[1]
        loads.append(
            pltpu.make_async_copy(
                stack.at[:, pl.ds(pl.multiple_of(my_narrow * rows, 16), rows), :],
                stage,
                load_sem.at[at],
            )
        )
        loads[-1].start()
    own = [
        pltpu.make_async_copy(features_ref, extended_ref.at[:, pl.ds(atoms, atoms), :], own_sem.at[0]),
        pltpu.make_async_copy(frames_ref, frames_v, own_sem.at[1]),
        pltpu.make_async_copy(radial_ref, radial_v, own_sem.at[2]),
    ]
    for copy in own:
        copy.start()

    total = wide * narrow
    me = my_wide * narrow + my_narrow
    after = lax.rem(me + 1, total)
    before = lax.rem(me + total - 1, total)
    place = lambda flat: (flat // narrow, lax.rem(flat, narrow))
    peers = [(lax.rem(my_wide + hop, wide), my_narrow) for hop in range(1, wide)]
    line = [(my_wide, lax.rem(my_narrow + hop, narrow)) for hop in range(1, narrow)]
    greeted = [place(after), place(before)] + peers + line
    barrier = pltpu.get_barrier_semaphore()
    for device in greeted:
        pl.semaphore_signal(barrier, inc=1, device_id=device, device_id_type=MESH)
    pl.semaphore_wait(barrier, len(greeted))

    halo = []
    for at, (degree, base, size) in enumerate(spans()):
        for side, device in enumerate([place(after), place(before)]):
            halo.append(
                remote(
                    features_ref.at[pl.ds(base, size)],
                    extended_ref.at[pl.ds(base, size), pl.ds(2 * side * atoms, atoms), :],
                    halo_send.at[2 * at + side],
                    halo_recv.at[2 * at + side],
                    device,
                )
            )
            halo[-1].start()

    offset = 0
    for load, stage in zip(loads, staged):
        load.wait()
        experts, rows, columns = stage.shape
        for block in range(columns // 128):
            lane = pl.ds(block * 128, 128)
            value = coefficient_ref[0] * stage[0, :, lane].astype(jnp.float32)
            for expert in range(1, experts):
                value = value + coefficient_ref[expert] * stage[expert, :, lane].astype(
                    jnp.float32
                )
            partial_ref[pl.ds(offset, rows), :] = value.astype(jnp.bfloat16)
            offset += rows
    if offset < partial_ref.shape[0]:
        rest = partial_ref.shape[0] - offset
        partial_ref[pl.ds(offset, rest), :] = jnp.zeros((rest, 128), jnp.bfloat16)

    scatter = []
    for hop, device in enumerate(peers):
        target = device[0]
        scatter.append(
            remote(
                partial_ref.at[pl.ds(pl.multiple_of(target * part, 16), part), :],
                received_ref.at[hop],
                send_sem.at[hop],
                recv_sem.at[hop],
                device,
            )
        )
        scatter[-1].start()

    everything = atoms * total
    relative = neighbours_ref[...] - (me * atoms - atoms)
    relative = jnp.where(relative < 0, relative + everything, relative)
    relative = jnp.where(relative >= everything, relative - everything, relative)
    relative = jnp.minimum(relative, 255)
    rows_ref[...] = relative.astype(jnp.float32).astype(jnp.bfloat16)
    for copy in own:
        copy.wait()

    def prepare(b, carried):
        edge = iota((1, lanes), 1) + b * lanes
        home = edge // slots
        slot = edge - home * slots
        chosen = (iota((atoms, lanes), 0) == home).astype(jnp.bfloat16)
        spread = jnp.dot(rows_ref[...], chosen, preferred_element_type=jnp.float32)
        index = jnp.sum(
            jnp.where(iota((slots, lanes), 0) == slot, spread, 0.0), axis=0, keepdims=True
        ).astype(jnp.int32)
        picked_ref[b] = (iota((extended, lanes), 0) == index).astype(jnp.bfloat16)
        row = pl.ds(pl.multiple_of(b * lanes, lanes), lanes)
        frame_t[b] = lax.dot_general(
            eye(frame_t.shape[1], entries),
            frames_v[row, :],
            ACROSS,
            preferred_element_type=jnp.float32,
        )
        radial_t[b] = lax.dot_general(
            eye(channels, channels), radial_v[row, :], ACROSS, preferred_element_type=jnp.float32
        ).astype(jnp.bfloat16)
        return carried

    lax.fori_loop(0, blocks, prepare, 0)

    summed = partial_ref[pl.ds(pl.multiple_of(my_wide * part, 16), part), :].astype(jnp.float32)
    for hop in range(wide - 1):
        scatter[hop].wait_recv()
        summed = summed + received_ref[hop].astype(jnp.float32)
    share_ref[...] = summed.astype(jnp.bfloat16)

    keep = pltpu.make_async_copy(share_ref, merged_ref.at[my_narrow, my_wide], local_sem)
    keep.start()
    partner = (my_wide + 1 - 2 * my_core, my_narrow)
    origin = lambda hop: lax.rem(my_narrow + narrow - hop, narrow)

    def line_copy(hop):
        return remote(
            share_ref,
            merged_ref.at[my_narrow, my_wide],
            line_send.at[hop - 1],
            line_recv.at[hop - 1],
            line[hop - 1],
        )

    def plane_copy(hop, step):
        slot = merged_ref.at[origin(hop), my_wide]
        at = hop * (chips - 1) + step - 1
        target = lax.rem(my_chip + step, chips) * 2 + my_core
        return remote(
            share_ref if hop == 0 else slot,
            slot,
            plane_send.at[at],
            plane_recv.at[at],
            (target, my_narrow),
        )

    def pair_copy(hop, step):
        owner = lax.rem(my_chip + chips - step, chips) * 2 + my_core
        slot = merged_ref.at[origin(hop), owner]
        at = hop * chips + step
        source = share_ref if hop == 0 and step == 0 else slot
        return remote(source, slot, pair_send.at[at], pair_recv.at[at], partner)

    def forward(hop):
        if hop:
            line_copy(hop).wait_recv()
        for step in range(1, chips):
            plane_copy(hop, step).start()
        pair_copy(hop, 0).start()

    def relay(hop):
        for step in range(1, chips):
            plane_copy(hop, step).wait_recv()
            pair_copy(hop, step).start()

    for hop in range(1, narrow):
        line_copy(hop).start()
    forward(0)

    steps = [functools.partial(forward, hop) for hop in range(1, narrow)]
    steps += [functools.partial(relay, hop) for hop in range(narrow)]
    ticks = dict(zip(plan, steps))
    rest = steps[len(plan) :]

    height = spread_ref.shape[1]
    for at, (degree, base, size) in enumerate(spans()):
        for side in range(2):
            halo[2 * at + side].wait_recv()
        for component in range(base, base + size):
            upright_ref[pl.ds(component * channels, channels), :] = jnp.transpose(
                extended_ref[component]
            )
        tall = pl.ds(base * channels, size * channels)
        first = sum((2 * d + 1) ** 2 for d in range(degree))

        def rotate(b, carried):
            for block, step in ticks.items():
                if block // blocks == at:
                    pl.when(b == block % blocks)(step)
            for q in range(size):
                source_ref[pl.ds(q * channels, channels), :] = jnp.dot(
                    upright_ref[pl.ds((base + q) * channels, channels), :],
                    picked_ref[b],
                    preferred_element_type=jnp.float32,
                ).astype(jnp.bfloat16)
            for k in range(size * size):
                row = frame_t[b, pl.ds(first + k, 1), :]
                spread_ref[k] = jnp.broadcast_to(row, spread_ref.shape[1:]).astype(jnp.bfloat16)
            for row in range(0, channels, height):
                scale = radial_t[b, pl.ds(row, height), :]
                xs = [source_ref[pl.ds(q * channels + row, height), :] for q in range(size)]
                for p in range(size):
                    value = spread_ref[p * size] * xs[0]
                    for q in range(1, size):
                        value = value + spread_ref[p * size + q] * xs[q]
                    kept_ref[b, pl.ds((base + p) * channels + row, height), :] = value * scale
            pltpu.make_async_copy(
                kept_ref.at[b, tall, :], turned_ref.at[b, tall, :], turned_sem.at[b, at]
            ).start()
            return carried

        lax.fori_loop(0, blocks, rotate, 0)

    for step in rest:
        step()
    for hop in range(narrow):
        for step in range(chips):
            pair_copy(hop, step).wait_recv()
    for hop in range(1, narrow):
        line_copy(hop).wait_send()
    for hop in range(narrow):
        for step in range(chips):
            pair_copy(hop, step).wait_send()
            if step:
                plane_copy(hop, step).wait_send()
    for copy in scatter + halo:
        copy.wait_send()
    keep.wait()
    for at, (degree, base, size) in enumerate(spans()):
        tall = pl.ds(base * channels, size * channels)
        for b in range(blocks):
            pltpu.make_async_copy(
                kept_ref.at[b, tall, :], turned_ref.at[b, tall, :], turned_sem.at[b, at]
            ).wait()


def exchange(features, frames, radial, neighbours, coefficients, stacks, lanes, plan):
    wide = lax.axis_size("wide")
    narrow = lax.axis_size("narrow")
    stacks = [flat_rows(w) for w in stacks]
    staged = [(w.shape[0], w.shape[1] // narrow, w.shape[2]) for w in stacks]
    rows = sum(shape[1] * shape[2] // 128 for shape in staged)
    unit = 16 * wide
    rows = -(-rows // unit) * unit
    part = rows // wide
    chips = wide // 2
    components, atoms, channels = features.shape
    edges, entries = frames.shape
    blocks = edges // lanes
    padded = -(-entries // 16) * 16
    height = 16
    anywhere = pl.BlockSpec(memory_space=pl.ANY)
    dma = lambda *n: pltpu.SemaphoreType.DMA(n)
    bf16 = lambda *shape: pltpu.VMEM(shape, jnp.bfloat16)
    widest = 2 * DEGREES - 1
    return pl.pallas_call(
        functools.partial(exchange_kernel, (wide, narrow, len(stacks)), plan),
        in_specs=[
            pl.BlockSpec(memory_space=pltpu.SMEM),
            pl.BlockSpec(memory_space=pltpu.VMEM),
        ]
        + [anywhere] * (3 + len(stacks)),
        out_specs=[anywhere, anywhere],
        out_shape=[
            jax.ShapeDtypeStruct((blocks, components * channels, lanes), jnp.bfloat16),
            jax.ShapeDtypeStruct((narrow, wide, part, 128), jnp.bfloat16),
        ],
        scratch_shapes=[bf16(*shape) for shape in staged]
        + [
            bf16(rows, 128),
            bf16(wide - 1, part, 128),
            bf16(part, 128),
            bf16(components, 3 * atoms, channels),
            bf16(components * channels, 3 * atoms),
            bf16(edges, entries),
            bf16(edges, channels),
            bf16(neighbours.shape[0], atoms),
            bf16(blocks, 3 * atoms, lanes),
            pltpu.VMEM((blocks, padded, lanes), jnp.float32),
            bf16(blocks, channels, lanes),
            bf16(widest * channels, lanes),
            bf16(widest * widest, height, lanes),
            bf16(blocks, components * channels, lanes),
            dma(len(stacks)),
            dma(3),
            dma(2 * DEGREES),
            dma(2 * DEGREES),
            dma(wide - 1),
            dma(wide - 1),
            dma(narrow - 1),
            dma(narrow - 1),
            dma(narrow * (chips - 1)),
            dma(narrow * (chips - 1)),
            dma(narrow * chips),
            dma(narrow * chips),
            pltpu.SemaphoreType.DMA,
            dma(blocks, DEGREES),
        ],
        compiler_params=pltpu.CompilerParams(
            collective_id=0, has_side_effects=True, vmem_limit_bytes=60 * 1024 * 1024
        ),
    )(coefficients, neighbours, features, frames, radial, *stacks)


def convolve_kernel(
    shapes,
    slots,
    counts_ref,
    frames_ref,
    turned_ref,
    merged_ref,
    out_ref,
    frame_ref,
    gated_ref,
    total_ref,
    column_ref,
    *weight_refs,
):
    step = pl.program_id(0)
    components, atoms, channels = out_ref.shape
    lanes, entries = frames_ref.shape
    members = merged_ref.shape[0]

    @pl.when(step == 0)
    def _():
        total_ref[...] = jnp.zeros_like(total_ref)
        square = (atoms, atoms)
        diagonal = iota(square, 0) == iota(square, 1)
        count = jnp.sum(
            jnp.where(diagonal, counts_ref[...].astype(jnp.float32), 0.0), axis=1, keepdims=True
        )
        column_ref[...] = jnp.broadcast_to(count, column_ref.shape)
        offset = 0
        for weight_ref, (rows, columns) in zip(weight_refs, shapes):
            part = rows // members
            for block in range(columns // 128):
                whole = jnp.concatenate(
                    [merged_ref[m, pl.ds(offset, part), :] for m in range(members)], axis=0
                )
                weight_ref[pl.ds(block * 128, 128), :] = jnp.transpose(whole)
                offset += part

    frame_ref[...] = lax.dot_general(
        eye(frame_ref.shape[0], entries),
        frames_ref[...],
        ACROSS,
        preferred_element_type=jnp.float32,
    )

    component_of = lambda degree, order: degree * degree + degree + order
    rows_of = lambda component: pl.ds(component * channels, channels)
    gather = lambda order: jnp.concatenate(
        [
            turned_ref[0, rows_of(component_of(degree, order)), :]
            for degree in range(abs(order), DEGREES)
        ],
        axis=0,
    )
    central = jnp.dot(weight_refs[0][...], gather(0), preferred_element_type=jnp.float32)
    gate = 1.0 / (1.0 + jnp.exp(-central[:channels]))
    for degree in range(DEGREES):
        gated_ref[rows_of(component_of(degree, 0)), :] = (
            central[degree * channels : (degree + 1) * channels] * gate
        ).astype(jnp.bfloat16)
    for order in range(1, DEGREES):
        plus = gather(order)
        minus = gather(-order)
        for side in range(2):
            pair = [plus, -minus] if side == 0 else [minus, plus]
            mixed = jnp.dot(
                weight_refs[order][...],
                jnp.concatenate(pair, axis=0),
                preferred_element_type=jnp.float32,
            )
            for column, degree in enumerate(range(order, DEGREES)):
                component = component_of(degree, order if side == 0 else -order)
                gated_ref[rows_of(component), :] = (
                    mixed[column * channels : (column + 1) * channels] * gate
                ).astype(jnp.bfloat16)

    edge = iota((1, lanes), 1) + step * lanes
    home = edge // slots
    slot = edge - home * slots
    window = 8
    first = jnp.minimum((step * lanes) // slots, atoms - window)
    position = slot + slots * (home - first) - slots * iota((window, lanes), 0)
    count = column_ref[pl.ds(first, window), :]
    count = jnp.concatenate([count] * (lanes // channels), axis=1)
    live = jnp.where(
        (position >= 0) & (position.astype(jnp.float32) < count) & (position < slots), 1.0, 0.0
    )
    offset = 0
    for degree in range(DEGREES):
        size = 2 * degree + 1
        summed = None
        for q in range(size):
            left = jnp.concatenate(
                [
                    jnp.broadcast_to(frame_ref[pl.ds(offset + q * size + p, 1), :], live.shape) * live
                    for p in range(size)
                ],
                axis=0,
            ).astype(jnp.bfloat16)
            term = lax.dot_general(
                left,
                gated_ref[rows_of(degree * degree + q), :],
                ACROSS,
                preferred_element_type=jnp.float32,
            )
            summed = term if summed is None else summed + term
        for p in range(size):
            at = degree * degree + p
            total_ref[at, pl.ds(first, window), :] = (
                total_ref[at, pl.ds(first, window), :] + summed[p * window : (p + 1) * window]
            )
        offset += size * size

    @pl.when(step == pl.num_programs(0) - 1)
    def _():
        scale = 1.0 / jnp.sqrt(column_ref[...])
        for component in range(components):
            out_ref[component] = total_ref[component] * scale


def body(
    node_features,
    frames,
    radial,
    neighbours,
    counts,
    coefficients,
    w_zero,
    w_one,
    w_two,
    w_three,
    w_four,
):
    atoms, components, channels = node_features.shape
    slots = neighbours.shape[1]
    entries = frames.shape[2]
    edges = atoms * slots
    stacks = (w_zero, w_one, w_two, w_three, w_four)
    lanes = 256
    features = node_features.transpose(1, 0, 2)
    frames = frames.reshape(edges, entries)
    turned, merged = exchange(
        features,
        frames,
        radial.reshape(edges, channels),
        neighbours.T,
        coefficients,
        stacks,
        lanes,
        PLAN,
    )
    merged = merged.reshape(merged.shape[0], -1, 128)
    shapes = [(int(np.prod(w.shape[1:-1])), w.shape[-1]) for w in stacks]

    padded = -(-entries // 16) * 16
    whole = lambda shape: pl.BlockSpec(shape, lambda i: (0,) * len(shape))
    out = pl.pallas_call(
        functools.partial(convolve_kernel, shapes, slots),
        grid=(edges // lanes,),
        in_specs=[
            whole((1, atoms)),
            pl.BlockSpec((lanes, entries), lambda i: (i, 0)),
            pl.BlockSpec((1, components * channels, lanes), lambda i: (i, 0, 0)),
            whole(merged.shape),
        ],
        out_specs=whole((components, atoms, channels)),
        out_shape=jax.ShapeDtypeStruct((components, atoms, channels), jnp.float32),
        scratch_shapes=[
            pltpu.VMEM((padded, lanes), jnp.float32),
            pltpu.VMEM((components * channels, lanes), jnp.bfloat16),
            pltpu.VMEM((components, atoms, channels), jnp.float32),
            pltpu.VMEM((atoms, channels), jnp.float32),
        ]
        + [pltpu.VMEM((n, k), jnp.bfloat16) for k, n in shapes],
        compiler_params=pltpu.CompilerParams(
            dimension_semantics=("arbitrary",), vmem_limit_bytes=56 * 1024 * 1024
        ),
    )(counts.reshape(1, atoms), frames, turned, merged)
    return out.transpose(1, 0, 2)


def solution(mesh):
    spread = lambda rest: P(AXES, *([None] * rest))
    in_specs = (
        spread(2),
        spread(2),
        spread(2),
        spread(1),
        spread(0),
        P("wide"),
        P("wide", None, None),
        P("wide", None, None, None),
        P("wide", None, None, None),
        P("wide", None, None, None),
        P("wide", None, None, None),
    )
    return jax.shard_map(body, mesh=mesh, in_specs=in_specs, out_specs=spread(2), check_vma=False)
```

```python
import functools

import jax
import jax.numpy as jnp
import numpy as np
from jax import lax
from jax.experimental import pallas as pl
from jax.experimental.pallas import tpu as pltpu
from jax.sharding import PartitionSpec as P

DEGREES = 5
COMPONENTS = DEGREES * DEGREES
AXES = ("wide", "narrow")
MESH = pl.DeviceIdType.MESH
EARLY = 2
PLAN = (8, 10, 16, 20, 22, 24, 28, 32, 36, 40, 44)


def flat_rows(weights):
    return weights.reshape(weights.shape[0], -1, weights.shape[-1])


def remote(src, dst, send, recv, device):
    return pltpu.make_async_remote_copy(
        src_ref=src,
        dst_ref=dst,
        send_sem=send,
        recv_sem=recv,
        device_id=device,
        device_id_type=MESH,
    )


def spans():
    return [(degree, degree * degree, 2 * degree + 1) for degree in reversed(range(DEGREES))]


def iota(shape, axis):
    return lax.broadcasted_iota(jnp.int32, shape, axis)


def eye(rows, columns):
    return (iota((rows, columns), 0) == iota((rows, columns), 1)).astype(jnp.bfloat16)


ACROSS = (((1,), (1,)), ((), ()))


def whole_kernel(sizes, shapes, plan, coefficient_ref, neighbours_ref, counts_ref, *refs):
    wide, narrow, count = sizes
    features_ref, frames_ref, radial_ref = refs[:3]
    refs = refs[3:]
    stacks = refs[:count]
    out_ref = refs[count]
    staged = refs[count + 1 : 2 * count + 1]
    weight_refs = refs[2 * count + 1 : 3 * count + 1]
    (
        partial_ref,
        received_ref,
        paired_ref,
        chip_ref,
        share_ref,
        extended_ref,
        upright_ref,
        frames_v,
        radial_v,
        rows_ref,
        picked_ref,
        frame_t,
        radial_t,
        source_ref,
        source_b,
        kept_ref,
        merged_ref,
        gated_ref,
        total_ref,
        column_ref,
        load_sem,
        own_sem,
        halo_send,
        halo_recv,
        send_sem,
        recv_sem,
        line_send,
        line_recv,
        plane_send,
        plane_recv,
        cross_send,
        cross_recv,
        pair_send,
        pair_recv,
        local_sem,
    ) = refs[3 * count + 1 :]
    my_wide = lax.axis_index("wide")
    my_narrow = lax.axis_index("narrow")
    part = partial_ref.shape[0] // wide
    chips = wide // 2
    my_chip = my_wide // 2
    my_core = lax.rem(my_wide, 2)
    slots, atoms = neighbours_ref.shape
    blocks, _, lanes = picked_ref.shape
    entries = frames_v.shape[1]
    channels = radial_v.shape[1]
    extended = extended_ref.shape[1]

    loads = []
    for at, (stack, stage) in enumerate(zip(stacks, staged)):
        rows = stage.shape[1]
        loads.append(
            pltpu.make_async_copy(
                stack.at[:, pl.ds(pl.multiple_of(my_narrow * rows, 16), rows), :],
                stage,
                load_sem.at[at],
            )
        )
        loads[-1].start()
    own = [
        pltpu.make_async_copy(features_ref, extended_ref.at[:, pl.ds(atoms, atoms), :], own_sem.at[0]),
        pltpu.make_async_copy(frames_ref, frames_v, own_sem.at[1]),
        pltpu.make_async_copy(radial_ref, radial_v, own_sem.at[2]),
    ]
    for copy in own:
        copy.start()

    total = wide * narrow
    me = my_wide * narrow + my_narrow
    after = lax.rem(me + 1, total)
    before = lax.rem(me + total - 1, total)
    place = lambda flat: (flat // narrow, lax.rem(flat, narrow))
    partner = (my_wide + 1 - 2 * my_core, my_narrow)
    peers = [
        (lax.rem(my_chip + hop, chips) * 2 + my_core, my_narrow) for hop in range(1, chips)
    ] + [partner]
    line = [(my_wide, lax.rem(my_narrow + hop, narrow)) for hop in range(1, narrow)]
    greeted = [place(after), place(before)] + peers + line
    barrier = pltpu.get_barrier_semaphore()
    for device in greeted:
        pl.semaphore_signal(barrier, inc=1, device_id=device, device_id_type=MESH)
    pl.semaphore_wait(barrier, len(greeted))

    def halo_copy(at, side):
        degree, base, size = spans()[at]
        return remote(
            features_ref.at[pl.ds(base, size)],
            extended_ref.at[pl.ds(base, size), pl.ds(2 * side * atoms, atoms), :],
            halo_send.at[2 * at + side],
            halo_recv.at[2 * at + side],
            [place(after), place(before)][side],
        )

    for at in range(EARLY):
        for side in range(2):
            halo_copy(at, side).start()

    offset = 0
    for load, stage in zip(loads, staged):
        load.wait()
        experts, rows, columns = stage.shape
        for block in range(columns // 128):
            lane = pl.ds(block * 128, 128)
            value = coefficient_ref[0] * stage[0, :, lane].astype(jnp.float32)
            for expert in range(1, experts):
                value = value + coefficient_ref[expert] * stage[expert, :, lane].astype(
                    jnp.float32
                )
            partial_ref[pl.ds(offset, rows), :] = value.astype(jnp.bfloat16)
            offset += rows
    if offset < partial_ref.shape[0]:
        rest = partial_ref.shape[0] - offset
        partial_ref[pl.ds(offset, rest), :] = jnp.zeros((rest, 128), jnp.bfloat16)

    half = chips * part
    theirs = pl.ds(pl.multiple_of((1 - my_core) * half, 16), half)
    pairing = remote(
        partial_ref.at[theirs, :], paired_ref, send_sem.at[0], recv_sem.at[0], partner
    )
    pairing.start()

    everything = atoms * total
    relative = neighbours_ref[...] - (me * atoms - atoms)
    relative = jnp.where(relative < 0, relative + everything, relative)
    relative = jnp.where(relative >= everything, relative - everything, relative)
    relative = jnp.minimum(relative, 255)
    rows_ref[...] = relative.astype(jnp.float32).astype(jnp.bfloat16)
    for copy in own:
        copy.wait()

    def prepare(b, carried):
        edge = iota((1, lanes), 1) + b * lanes
        home = edge // slots
        slot = edge - home * slots
        chosen = (iota((atoms, lanes), 0) == home).astype(jnp.bfloat16)
        spread = jnp.dot(rows_ref[...], chosen, preferred_element_type=jnp.float32)
        index = jnp.sum(
            jnp.where(iota((slots, lanes), 0) == slot, spread, 0.0), axis=0, keepdims=True
        ).astype(jnp.int32)
        picked_ref[b] = (iota((extended, lanes), 0) == index).astype(jnp.bfloat16)
        row = pl.ds(pl.multiple_of(b * lanes, lanes), lanes)
        frame_t[b] = lax.dot_general(
            eye(frame_t.shape[1], entries),
            frames_v[row, :],
            ACROSS,
            preferred_element_type=jnp.float32,
        )
        scales = lax.dot_general(
            eye(channels, channels), radial_v[row, :], ACROSS, preferred_element_type=jnp.float32
        ).astype(jnp.bfloat16)
        radial_t[b] = scales.reshape(radial_t.shape[1:])
        return carried

    lax.fori_loop(0, blocks // 4, prepare, 0)

    pairing.wait_recv()
    scatter = []
    for hop in range(1, chips):
        target = lax.rem(my_chip + hop, chips)
        mine = pl.ds(pl.multiple_of(my_core * half + target * part, 16), part)
        there = pl.ds(pl.multiple_of(target * part, 16), part)
        chip_ref[hop - 1] = (
            partial_ref[mine, :].astype(jnp.float32) + paired_ref[there, :].astype(jnp.float32)
        ).astype(jnp.bfloat16)
        scatter.append(
            remote(
                chip_ref.at[hop - 1],
                received_ref.at[hop - 1],
                send_sem.at[hop],
                recv_sem.at[hop],
                (target * 2 + my_core, my_narrow),
            )
        )
        scatter[-1].start()
    lax.fori_loop(blocks // 4, blocks, prepare, 0)
    mine = pl.ds(pl.multiple_of(my_core * half + my_chip * part, 16), part)
    there = pl.ds(pl.multiple_of(my_chip * part, 16), part)
    summed = partial_ref[mine, :].astype(jnp.float32) + paired_ref[there, :].astype(jnp.float32)
    for hop in range(chips - 1):
        scatter[hop].wait_recv()
        summed = summed + received_ref[hop].astype(jnp.float32)
    share_ref[...] = summed.astype(jnp.bfloat16)

    my_place = my_core * chips + my_chip
    keep = pltpu.make_async_copy(share_ref, merged_ref.at[my_narrow, pl.ds(pl.multiple_of(my_place * part, 16), part), :], local_sem)
    keep.start()
    origin = lambda hop: lax.rem(my_narrow + narrow - hop, narrow)

    square = chips == 4
    if square:
        hops = [my_chip + 1 - 2 * lax.rem(my_chip, 2), my_chip + 2 - 4 * (my_chip // 2)]
        far = lax.rem(my_chip + 1, 2) + 2 * (1 - my_chip // 2)
        sources = hops
        owners = [my_chip] + hops + [far]
    else:
        hops = [lax.rem(my_chip + step, chips) for step in range(1, chips)]
        sources = [lax.rem(my_chip + chips - step, chips) for step in range(1, chips)]
        owners = [my_chip] + sources

    def spot(hop, chip, start=0, rows=part):
        row = (my_core * chips + chip) * part + start
        return merged_ref.at[origin(hop), pl.ds(pl.multiple_of(row, 16), rows), :]


    def line_copy(hop):
        return remote(
            share_ref,
            merged_ref.at[my_narrow, pl.ds(pl.multiple_of(my_place * part, 16), part), :],
            line_send.at[hop - 1],
            line_recv.at[hop - 1],
            line[hop - 1],
        )

    def plane_copy(hop, way):
        slot = spot(hop, my_chip)
        at = hop * len(hops) + way
        return remote(
            share_ref if hop == 0 else slot,
            slot,
            plane_send.at[at],
            plane_recv.at[at],
            (hops[way] * 2 + my_core, my_narrow),
        )

    def cross_copy(hop, way):
        slot = spot(hop, hops[way], way * cut, cut if way == 0 else part - cut)
        at = hop * 2 + way
        return remote(
            slot,
            slot,
            cross_send.at[at],
            cross_recv.at[at],
            (hops[1 - way] * 2 + my_core, my_narrow),
        )

    cut = part // 32 * 16

    def crossed(hop, way):
        slot = spot(hop, far, way * cut, cut if way == 0 else part - cut)
        at = hop * 2 + way
        return remote(
            slot,
            slot,
            cross_send.at[at],
            cross_recv.at[at],
            (hops[1 - way] * 2 + my_core, my_narrow),
        )

    def pair_copy(hop, step):
        slot = spot(hop, owners[step])
        at = hop * chips + step
        source = share_ref if hop == 0 and step == 0 else slot
        return remote(source, slot, pair_send.at[at], pair_recv.at[at], partner)

    def forward(hop):
        if hop:
            line_copy(hop).wait_recv()
        for way in range(len(hops)):
            plane_copy(hop, way).start()
        pair_copy(hop, 0).start()

    def relay(hop):
        for way in range(len(hops)):
            plane_copy(hop, way).wait_recv()
            if square:
                cross_copy(hop, way).start()
            pair_copy(hop, way + 1).start()

    def close(hop):
        for way in range(2):
            crossed(hop, way).wait_recv()
        pair_copy(hop, 3).start()

    for hop in range(1, narrow):
        line_copy(hop).start()
    for at in range(EARLY, DEGREES):
        for side in range(2):
            halo_copy(at, side).start()
    forward(0)

    steps = []
    for turn in range(narrow + 2):
        if 0 < turn < narrow:
            steps.append(functools.partial(forward, turn))
        if 0 < turn <= narrow:
            steps.append(functools.partial(relay, turn - 1))
        if square and turn > 1:
            steps.append(functools.partial(close, turn - 2))
    ticks = dict(zip(plan, steps))
    rest = steps[len(plan) :]

    groups, height = radial_t.shape[1:3]
    for at, (degree, base, size) in enumerate(spans()):
        for side in range(2):
            halo_copy(at, side).wait_recv()
        for component in range(base, base + size):
            upright_ref[component] = jnp.transpose(extended_ref[component]).reshape(
                upright_ref.shape[1:]
            )
        first = sum((2 * d + 1) ** 2 for d in range(degree))

        def fetch(b, group, source):
            left = jnp.concatenate(
                [upright_ref[base + q, group] for q in range(size)], axis=0
            )
            got = jnp.dot(left, picked_ref[b], preferred_element_type=jnp.float32)
            for q in range(size):
                source[q, group] = got[q * height : (q + 1) * height].astype(jnp.bfloat16)

        def rotate(b, group, source):
            for lane in range(0, lanes, 128):
                part_of = pl.ds(lane, 128)

                def entry(k):
                    row = frame_t[b, pl.ds(first + k, 1), part_of]
                    row = jnp.broadcast_to(row, (16, 128)).astype(jnp.bfloat16)
                    return jnp.concatenate([row] * (height // 16), axis=0)

                scale = radial_t[b, group, :, part_of]
                xs = [source[q, group, :, part_of] for q in range(size)]
                for p in range(size):
                    value = entry(p * size) * xs[0]
                    for q in range(1, size):
                        value = value + entry(p * size + q) * xs[q]
                    kept_ref[b, base + p, group, :, part_of] = value * scale

        def all_groups(work):
            if size > 5:
                lax.fori_loop(0, groups, lambda group, carried: (work(group), carried)[1], 0)
            else:
                for group in range(groups):
                    work(group)

        buffers = [source_ref, source_b]
        all_groups(lambda group: fetch(0, group, buffers[0]))

        def pair(i, carried):
            for block, step in ticks.items():
                if block // blocks == at:
                    pl.when(i == block % blocks // 2)(step)
            for k in range(2):
                b = 2 * i + k
                following = jnp.minimum(b + 1, blocks - 1)

                def both(group, b=b, following=following, k=k):
                    fetch(following, group, buffers[1 - k])
                    rotate(b, group, buffers[k])

                all_groups(both)
            return carried

        lax.fori_loop(0, blocks // 2, pair, 0)

    for step in rest:
        step()
    for hop in range(narrow):
        for step in range(chips):
            pair_copy(hop, step).wait_recv()
    for hop in range(1, narrow):
        line_copy(hop).wait_send()
    for hop in range(narrow):
        for step in range(chips):
            pair_copy(hop, step).wait_send()
        for way in range(len(hops)):
            plane_copy(hop, way).wait_send()
            if square:
                cross_copy(hop, way).wait_send()
    for copy in scatter + [pairing]:
        copy.wait_send()
    for at in range(DEGREES):
        for side in range(2):
            halo_copy(at, side).wait_send()
    keep.wait()

    offset = 0
    for weight_ref, (rows, columns) in zip(weight_refs, shapes):
        piece = rows // narrow
        for block in range(columns // 128):
            gathered = jnp.concatenate(
                [merged_ref[m, pl.ds(offset, piece), :] for m in range(narrow)], axis=0
            )
            weight_ref[pl.ds(block * 128, 128), :] = jnp.transpose(gathered)
            offset += piece
    total_ref[...] = jnp.zeros_like(total_ref)
    square = (atoms, atoms)
    diagonal = iota(square, 0) == iota(square, 1)
    count = jnp.sum(
        jnp.where(diagonal, counts_ref[...].astype(jnp.float32), 0.0), axis=1, keepdims=True
    )
    column_ref[...] = jnp.broadcast_to(count, column_ref.shape)

    def mix(b, carried):
        mix_block(b, slots, kept_ref, frame_t, weight_refs, gated_ref, total_ref, column_ref)
        return carried

    lax.fori_loop(0, blocks, mix, 0)

    scale = 1.0 / jnp.sqrt(column_ref[...])
    for component in range(COMPONENTS):
        out_ref[component] = total_ref[component] * scale


def mix_block(b, slots, kept_ref, frame_t, weight_refs, gated_ref, total_ref, column_ref):
    atoms, channels = column_ref.shape
    lanes = gated_ref.shape[1]
    component_of = lambda degree, order: degree * degree + degree + order
    rows_of = lambda component: pl.ds(component * channels, channels)
    gather = lambda order: jnp.concatenate(
        [
            kept_ref[b, component_of(degree, order)].reshape(channels, lanes)
            for degree in range(abs(order), DEGREES)
        ],
        axis=0,
    )
    central = jnp.dot(weight_refs[0][...], gather(0), preferred_element_type=jnp.float32)
    gate = 1.0 / (1.0 + jnp.exp(-central[:channels]))
    for degree in range(DEGREES):
        gated_ref[rows_of(component_of(degree, 0)), :] = (
            central[degree * channels : (degree + 1) * channels] * gate
        ).astype(jnp.bfloat16)
    for order in range(1, DEGREES):
        plus = gather(order)
        minus = gather(-order)
        for side in range(2):
            pair = [plus, -minus] if side == 0 else [minus, plus]
            mixed = jnp.dot(
                weight_refs[order][...],
                jnp.concatenate(pair, axis=0),
                preferred_element_type=jnp.float32,
            )
            for column, degree in enumerate(range(order, DEGREES)):
                component = component_of(degree, order if side == 0 else -order)
                gated_ref[rows_of(component), :] = (
                    mixed[column * channels : (column + 1) * channels] * gate
                ).astype(jnp.bfloat16)

    edge = iota((1, lanes), 1) + b * lanes
    home = edge // slots
    slot = edge - home * slots
    window = 8
    first = jnp.minimum((b * lanes) // slots, atoms - window)
    position = slot + slots * (home - first) - slots * iota((window, lanes), 0)
    count = column_ref[pl.ds(first, window), :]
    count = jnp.concatenate([count] * (lanes // channels), axis=1)
    live = jnp.where(
        (position >= 0) & (position.astype(jnp.float32) < count) & (position < slots), 1.0, 0.0
    )
    offset = 0
    for degree in range(DEGREES):
        size = 2 * degree + 1
        summed = None
        for q in range(size):
            left = jnp.concatenate(
                [
                    jnp.broadcast_to(frame_t[b, pl.ds(offset + q * size + p, 1), :], live.shape)
                    * live
                    for p in range(size)
                ],
                axis=0,
            ).astype(jnp.bfloat16)
            term = lax.dot_general(
                left,
                gated_ref[rows_of(degree * degree + q), :],
                ACROSS,
                preferred_element_type=jnp.float32,
            )
            summed = term if summed is None else summed + term
        for p in range(size):
            at = degree * degree + p
            total_ref[at, pl.ds(first, window), :] = (
                total_ref[at, pl.ds(first, window), :] + summed[p * window : (p + 1) * window]
            )
        offset += size * size


def run(features, frames, radial, neighbours, counts, coefficients, stacks, lanes, plan):
    shapes = [(int(np.prod(w.shape[1:-1])), w.shape[-1]) for w in stacks]
    wide = lax.axis_size("wide")
    narrow = lax.axis_size("narrow")
    stacks = [flat_rows(w) for w in stacks]
    staged = [(w.shape[0], w.shape[1] // narrow, w.shape[2]) for w in stacks]
    rows = sum(shape[1] * shape[2] // 128 for shape in staged)
    unit = 16 * wide
    rows = -(-rows // unit) * unit
    part = rows // wide
    chips = wide // 2
    components, atoms, channels = features.shape
    edges, entries = frames.shape
    blocks = edges // lanes
    padded = -(-entries // 16) * 16
    groups = 2
    height = channels // groups
    anywhere = pl.BlockSpec(memory_space=pl.ANY)
    vmem = pl.BlockSpec(memory_space=pltpu.VMEM)
    dma = lambda *n: pltpu.SemaphoreType.DMA(n)
    bf16 = lambda *shape: pltpu.VMEM(shape, jnp.bfloat16)
    widest = 2 * DEGREES - 1
    return pl.pallas_call(
        functools.partial(whole_kernel, (wide, narrow, len(stacks)), shapes, plan),
        in_specs=[pl.BlockSpec(memory_space=pltpu.SMEM), vmem, vmem]
        + [anywhere] * (3 + len(stacks)),
        out_specs=vmem,
        out_shape=jax.ShapeDtypeStruct((components, atoms, channels), jnp.float32),
        scratch_shapes=[bf16(*shape) for shape in staged]
        + [bf16(n, k) for k, n in shapes]
        + [
            bf16(rows, 128),
            bf16(chips - 1, part, 128),
            bf16(chips * part, 128),
            bf16(chips - 1, part, 128),
            bf16(part, 128),
            bf16(components, 3 * atoms, channels),
            bf16(components, groups, height, 3 * atoms),
            bf16(edges, entries),
            bf16(edges, channels),
            bf16(neighbours.shape[0], atoms),
            bf16(blocks, 3 * atoms, lanes),
            pltpu.VMEM((blocks, padded, lanes), jnp.float32),
            bf16(blocks, groups, height, lanes),
            bf16(widest, groups, height, lanes),
            bf16(widest, groups, height, lanes),
            bf16(blocks, components, groups, height, lanes),
            bf16(narrow, wide * part, 128),
            bf16(components * channels, lanes),
            pltpu.VMEM((components, atoms, channels), jnp.float32),
            pltpu.VMEM((atoms, channels), jnp.float32),
            dma(len(stacks)),
            dma(3),
            dma(2 * DEGREES),
            dma(2 * DEGREES),
            dma(chips),
            dma(chips),
            dma(narrow - 1),
            dma(narrow - 1),
            dma(narrow * (chips - 1)),
            dma(narrow * (chips - 1)),
            dma(narrow * 2),
            dma(narrow * 2),
            dma(narrow * chips),
            dma(narrow * chips),
            pltpu.SemaphoreType.DMA,
        ],
        compiler_params=pltpu.CompilerParams(
            collective_id=0, has_side_effects=True, vmem_limit_bytes=60 * 1024 * 1024
        ),
    )(coefficients, neighbours, counts, features, frames, radial, *stacks)


def body(
    node_features,
    frames,
    radial,
    neighbours,
    counts,
    coefficients,
    w_zero,
    w_one,
    w_two,
    w_three,
    w_four,
):
    atoms, components, channels = node_features.shape
    slots = neighbours.shape[1]
    entries = frames.shape[2]
    edges = atoms * slots
    stacks = (w_zero, w_one, w_two, w_three, w_four)
    lanes = 256
    features = node_features.transpose(1, 0, 2)
    frames = frames.reshape(edges, entries)
    out = run(
        features,
        frames,
        radial.reshape(edges, channels),
        neighbours.T,
        counts.reshape(1, atoms),
        coefficients,
        stacks,
        lanes,
        PLAN,
    )
    return out.transpose(1, 0, 2)


def solution(mesh):
    spread = lambda rest: P(AXES, *([None] * rest))
    in_specs = (
        spread(2),
        spread(2),
        spread(2),
        spread(1),
        spread(0),
        P("wide"),
        P("wide", None, None),
        P("wide", None, None, None),
        P("wide", None, None, None),
        P("wide", None, None, None),
        P("wide", None, None, None),
    )
    return jax.shard_map(body, mesh=mesh, in_specs=in_specs, out_specs=spread(2), check_vma=False)
```

```python
import functools

import jax
import jax.numpy as jnp
import numpy as np
from jax import lax
from jax.experimental import pallas as pl
from jax.experimental.pallas import tpu as pltpu
from jax.sharding import PartitionSpec as P

DEGREES = 5
COMPONENTS = DEGREES * DEGREES
AXES = ("wide", "narrow")
THREE = (1, 3)
MESH = pl.DeviceIdType.MESH
EARLY = 2
PLAN = (8, 10, 16, 20, 22, 24, 28, 32, 36, 40, 44)


def flat_rows(weights):
    return weights.reshape(weights.shape[0], -1, weights.shape[-1])


def remote(src, dst, send, recv, device):
    return pltpu.make_async_remote_copy(
        src_ref=src,
        dst_ref=dst,
        send_sem=send,
        recv_sem=recv,
        device_id=device,
        device_id_type=MESH,
    )


def spans():
    return [(degree, degree * degree, 2 * degree + 1) for degree in reversed(range(DEGREES))]


def iota(shape, axis):
    return lax.broadcasted_iota(jnp.int32, shape, axis)


def eye(rows, columns):
    return (iota((rows, columns), 0) == iota((rows, columns), 1)).astype(jnp.bfloat16)


ACROSS = (((1,), (1,)), ((), ()))


def whole_kernel(sizes, shapes, plan, coefficient_ref, neighbours_ref, counts_ref, *refs):
    wide, narrow, count = sizes
    features_ref, frames_ref, radial_ref = refs[:3]
    refs = refs[3:]
    stacks = refs[:count]
    out_ref = refs[count]
    staged = refs[count + 1 : 2 * count + 1]
    weight_refs = refs[2 * count + 1 : 3 * count + 1]
    (
        partial_ref,
        received_ref,
        paired_ref,
        chip_ref,
        share_ref,
        extended_ref,
        upright_ref,
        frames_v,
        radial_v,
        rows_ref,
        picked_ref,
        frame_t,
        radial_t,
        source_ref,
        source_b,
        kept_ref,
        merged_ref,
        gated_ref,
        total_ref,
        column_ref,
        load_sem,
        own_sem,
        halo_send,
        halo_recv,
        send_sem,
        recv_sem,
        line_send,
        line_recv,
        plane_send,
        plane_recv,
        cross_send,
        cross_recv,
        pair_send,
        pair_recv,
        local_sem,
    ) = refs[3 * count + 1 :]
    my_wide = lax.axis_index("wide")
    my_narrow = lax.axis_index("narrow")
    part = partial_ref.shape[0] // wide
    chips = wide // 2
    my_chip = my_wide // 2
    my_core = lax.rem(my_wide, 2)
    slots, atoms = neighbours_ref.shape
    blocks, _, lanes = picked_ref.shape
    entries = frames_v.shape[1]
    channels = radial_v.shape[1]
    extended = extended_ref.shape[1]

    loads = []
    for at, (stack, stage) in enumerate(zip(stacks, staged)):
        rows = stage.shape[1]
        loads.append(
            pltpu.make_async_copy(
                stack.at[:, pl.ds(pl.multiple_of(my_narrow * rows, 16), rows), :],
                stage,
                load_sem.at[at],
            )
        )
        loads[-1].start()
    own = [
        pltpu.make_async_copy(features_ref, extended_ref.at[:, pl.ds(atoms, atoms), :], own_sem.at[0]),
        pltpu.make_async_copy(frames_ref, frames_v, own_sem.at[1]),
        pltpu.make_async_copy(radial_ref, radial_v, own_sem.at[2]),
    ]
    for copy in own:
        copy.start()

    total = wide * narrow
    me = my_wide * narrow + my_narrow
    after = lax.rem(me + 1, total)
    before = lax.rem(me + total - 1, total)
    place = lambda flat: (flat // narrow, lax.rem(flat, narrow))
    partner = (my_wide + 1 - 2 * my_core, my_narrow)
    peers = [
        (lax.rem(my_chip + hop, chips) * 2 + my_core, my_narrow) for hop in range(1, chips)
    ] + [partner]
    line = [(my_wide, lax.rem(my_narrow + hop, narrow)) for hop in range(1, narrow)]
    greeted = [place(after), place(before)] + peers + line
    barrier = pltpu.get_barrier_semaphore()
    for device in greeted:
        pl.semaphore_signal(barrier, inc=1, device_id=device, device_id_type=MESH)
    pl.semaphore_wait(barrier, len(greeted))

    def halo_copy(at, side):
        degree, base, size = spans()[at]
        return remote(
            features_ref.at[pl.ds(base, size)],
            extended_ref.at[pl.ds(base, size), pl.ds(2 * side * atoms, atoms), :],
            halo_send.at[2 * at + side],
            halo_recv.at[2 * at + side],
            [place(after), place(before)][side],
        )

    for at in range(EARLY):
        for side in range(2):
            halo_copy(at, side).start()

    offset = 0
    for load, stage in zip(loads, staged):
        load.wait()
        experts, rows, columns = stage.shape
        for block in range(columns // 128):
            lane = pl.ds(block * 128, 128)
            value = coefficient_ref[0] * stage[0, :, lane].astype(jnp.float32)
            for expert in range(1, experts):
                value = value + coefficient_ref[expert] * stage[expert, :, lane].astype(
                    jnp.float32
                )
            partial_ref[pl.ds(offset, rows), :] = value.astype(jnp.bfloat16)
            offset += rows
    if offset < partial_ref.shape[0]:
        rest = partial_ref.shape[0] - offset
        partial_ref[pl.ds(offset, rest), :] = jnp.zeros((rest, 128), jnp.bfloat16)

    half = chips * part
    theirs = pl.ds(pl.multiple_of((1 - my_core) * half, 16), half)
    pairing = remote(
        partial_ref.at[theirs, :], paired_ref, send_sem.at[0], recv_sem.at[0], partner
    )
    pairing.start()

    everything = atoms * total
    relative = neighbours_ref[...] - (me * atoms - atoms)
    relative = jnp.where(relative < 0, relative + everything, relative)
    relative = jnp.where(relative >= everything, relative - everything, relative)
    relative = jnp.minimum(relative, 255)
    rows_ref[...] = relative.astype(jnp.float32).astype(jnp.bfloat16)
    for copy in own:
        copy.wait()

    def prepare(b, carried):
        edge = iota((1, lanes), 1) + b * lanes
        home = edge // slots
        slot = edge - home * slots
        chosen = (iota((atoms, lanes), 0) == home).astype(jnp.bfloat16)
        spread = jnp.dot(rows_ref[...], chosen, preferred_element_type=jnp.float32)
        index = jnp.sum(
            jnp.where(iota((slots, lanes), 0) == slot, spread, 0.0), axis=0, keepdims=True
        ).astype(jnp.int32)
        picked_ref[b] = (iota((extended, lanes), 0) == index).astype(jnp.bfloat16)
        row = pl.ds(pl.multiple_of(b * lanes, lanes), lanes)
        frame_t[b] = lax.dot_general(
            eye(frame_t.shape[1], entries),
            frames_v[row, :],
            ACROSS,
            preferred_element_type=jnp.float32,
        )
        scales = lax.dot_general(
            eye(channels, channels), radial_v[row, :], ACROSS, preferred_element_type=jnp.float32
        ).astype(jnp.bfloat16)
        radial_t[b] = scales.reshape(radial_t.shape[1:])
        return carried

    lax.fori_loop(0, blocks // 4, prepare, 0)

    pairing.wait_recv()
    scatter = []
    for hop in range(1, chips):
        target = lax.rem(my_chip + hop, chips)
        mine = pl.ds(pl.multiple_of(my_core * half + target * part, 16), part)
        there = pl.ds(pl.multiple_of(target * part, 16), part)
        chip_ref[hop - 1] = (
            partial_ref[mine, :].astype(jnp.float32) + paired_ref[there, :].astype(jnp.float32)
        ).astype(jnp.bfloat16)
        scatter.append(
            remote(
                chip_ref.at[hop - 1],
                received_ref.at[hop - 1],
                send_sem.at[hop],
                recv_sem.at[hop],
                (target * 2 + my_core, my_narrow),
            )
        )
        scatter[-1].start()
    lax.fori_loop(blocks // 4, blocks, prepare, 0)
    mine = pl.ds(pl.multiple_of(my_core * half + my_chip * part, 16), part)
    there = pl.ds(pl.multiple_of(my_chip * part, 16), part)
    summed = partial_ref[mine, :].astype(jnp.float32) + paired_ref[there, :].astype(jnp.float32)
    for hop in range(chips - 1):
        scatter[hop].wait_recv()
        summed = summed + received_ref[hop].astype(jnp.float32)
    share_ref[...] = summed.astype(jnp.bfloat16)

    my_place = my_core * chips + my_chip
    keep = pltpu.make_async_copy(share_ref, merged_ref.at[my_narrow, pl.ds(pl.multiple_of(my_place * part, 16), part), :], local_sem)
    keep.start()
    origin = lambda hop: lax.rem(my_narrow + narrow - hop, narrow)

    square = chips == 4
    if square:
        hops = [my_chip + 1 - 2 * lax.rem(my_chip, 2), my_chip + 2 - 4 * (my_chip // 2)]
        far = lax.rem(my_chip + 1, 2) + 2 * (1 - my_chip // 2)
        sources = hops
        owners = [my_chip] + hops + [far]
    else:
        hops = [lax.rem(my_chip + step, chips) for step in range(1, chips)]
        sources = [lax.rem(my_chip + chips - step, chips) for step in range(1, chips)]
        owners = [my_chip] + sources

    def spot(hop, chip, start=0, rows=part):
        row = (my_core * chips + chip) * part + start
        return merged_ref.at[origin(hop), pl.ds(pl.multiple_of(row, 16), rows), :]


    def line_copy(hop):
        return remote(
            share_ref,
            merged_ref.at[my_narrow, pl.ds(pl.multiple_of(my_place * part, 16), part), :],
            line_send.at[hop - 1],
            line_recv.at[hop - 1],
            line[hop - 1],
        )

    def plane_copy(hop, way):
        slot = spot(hop, my_chip)
        at = hop * len(hops) + way
        return remote(
            share_ref if hop == 0 else slot,
            slot,
            plane_send.at[at],
            plane_recv.at[at],
            (hops[way] * 2 + my_core, my_narrow),
        )

    def cross_copy(hop, way):
        slot = spot(hop, hops[way], way * cut, cut if way == 0 else part - cut)
        at = hop * 2 + way
        return remote(
            slot,
            slot,
            cross_send.at[at],
            cross_recv.at[at],
            (hops[1 - way] * 2 + my_core, my_narrow),
        )

    cut = part // 32 * 16

    def crossed(hop, way):
        slot = spot(hop, far, way * cut, cut if way == 0 else part - cut)
        at = hop * 2 + way
        return remote(
            slot,
            slot,
            cross_send.at[at],
            cross_recv.at[at],
            (hops[1 - way] * 2 + my_core, my_narrow),
        )

    def pair_copy(hop, step):
        slot = spot(hop, owners[step])
        at = hop * chips + step
        source = share_ref if hop == 0 and step == 0 else slot
        return remote(source, slot, pair_send.at[at], pair_recv.at[at], partner)

    def forward(hop):
        if hop:
            line_copy(hop).wait_recv()
        for way in range(len(hops)):
            plane_copy(hop, way).start()
        pair_copy(hop, 0).start()

    def relay(hop):
        for way in range(len(hops)):
            plane_copy(hop, way).wait_recv()
            if square:
                cross_copy(hop, way).start()
            pair_copy(hop, way + 1).start()

    def close(hop):
        for way in range(2):
            crossed(hop, way).wait_recv()
        pair_copy(hop, 3).start()

    for hop in range(1, narrow):
        line_copy(hop).start()
    for at in range(EARLY, DEGREES):
        for side in range(2):
            halo_copy(at, side).start()
    forward(0)

    steps = []
    for turn in range(narrow + 2):
        if 0 < turn < narrow:
            steps.append(functools.partial(forward, turn))
        if 0 < turn <= narrow:
            steps.append(functools.partial(relay, turn - 1))
        if square and turn > 1:
            steps.append(functools.partial(close, turn - 2))
    ticks = dict(zip(plan, steps))
    rest = steps[len(plan) :]

    groups, height = radial_t.shape[1:3]
    for at, (degree, base, size) in enumerate(spans()):
        for side in range(2):
            halo_copy(at, side).wait_recv()
        for component in range(base, base + size):
            upright_ref[component] = jnp.transpose(extended_ref[component]).reshape(
                upright_ref.shape[1:]
            )
        first = sum((2 * d + 1) ** 2 for d in range(degree))

        def fetch(b, group, source):
            left = jnp.concatenate(
                [upright_ref[base + q, group] for q in range(size)], axis=0
            )
            got = jnp.dot(left, picked_ref[b], preferred_element_type=jnp.float32)
            for q in range(size):
                source[q, group] = got[q * height : (q + 1) * height].astype(jnp.bfloat16)

        def rotate(b, group, source):
            for lane in range(0, lanes, 128):
                part_of = pl.ds(lane, 128)

                def entry(k):
                    row = frame_t[b, pl.ds(first + k, 1), part_of]
                    row = jnp.broadcast_to(row, (16, 128)).astype(jnp.bfloat16)
                    return jnp.concatenate([row] * (height // 16), axis=0)

                scale = radial_t[b, group, :, part_of]
                xs = [source[q, group, :, part_of] for q in range(size)]
                for p in range(size):
                    value = entry(p * size) * xs[0]
                    for q in range(1, size):
                        value = value + entry(p * size + q) * xs[q]
                    kept_ref[b, base + p, group, :, part_of] = value * scale

        def all_groups(work):
            if size > 5:
                lax.fori_loop(0, groups, lambda group, carried: (work(group), carried)[1], 0)
            else:
                for group in range(groups):
                    work(group)

        buffers = [source_ref, source_b]
        all_groups(lambda group: fetch(0, group, buffers[0]))

        def pair(i, carried):
            for block, step in ticks.items():
                if block // blocks == at:
                    pl.when(i == block % blocks // 2)(step)
            for k in range(2):
                b = 2 * i + k
                following = jnp.minimum(b + 1, blocks - 1)

                def both(group, b=b, following=following, k=k):
                    fetch(following, group, buffers[1 - k])
                    rotate(b, group, buffers[k])

                all_groups(both)
            return carried

        lax.fori_loop(0, blocks // 2, pair, 0)

    for step in rest:
        step()
    for hop in range(narrow):
        for step in range(chips):
            pair_copy(hop, step).wait_recv()
    for hop in range(1, narrow):
        line_copy(hop).wait_send()
    for hop in range(narrow):
        for step in range(chips):
            pair_copy(hop, step).wait_send()
        for way in range(len(hops)):
            plane_copy(hop, way).wait_send()
            if square:
                cross_copy(hop, way).wait_send()
    for copy in scatter + [pairing]:
        copy.wait_send()
    for at in range(DEGREES):
        for side in range(2):
            halo_copy(at, side).wait_send()
    keep.wait()

    offset = 0
    for order, (weight_ref, (rows, columns)) in enumerate(zip(weight_refs, shapes)):
        piece = rows // narrow
        for block in range(columns // 128):
            gathered = jnp.concatenate(
                [merged_ref[m, pl.ds(offset, piece), :] for m in range(narrow)], axis=0
            )
            if order in THREE:
                real = gathered[: rows // 2].astype(jnp.float32)
                imag = gathered[rows // 2 :].astype(jnp.float32)
                gathered = jnp.concatenate([real, real + imag, imag - real], axis=0).astype(
                    jnp.bfloat16
                )
            weight_ref[pl.ds(block * 128, 128), :] = jnp.transpose(gathered)
            offset += piece
    total_ref[...] = jnp.zeros_like(total_ref)
    square = (atoms, atoms)
    diagonal = iota(square, 0) == iota(square, 1)
    count = jnp.sum(
        jnp.where(diagonal, counts_ref[...].astype(jnp.float32), 0.0), axis=1, keepdims=True
    )
    column_ref[...] = jnp.broadcast_to(count, column_ref.shape)

    def mix(b, carried):
        mix_block(b, slots, kept_ref, frame_t, weight_refs, gated_ref, total_ref, column_ref)
        return carried

    lax.fori_loop(0, blocks, mix, 0)

    scale = 1.0 / jnp.sqrt(column_ref[...])
    for component in range(COMPONENTS):
        out_ref[component] = total_ref[component] * scale


def mix_block(b, slots, kept_ref, frame_t, weight_refs, gated_ref, total_ref, column_ref):
    atoms, channels = column_ref.shape
    lanes = gated_ref.shape[1]
    component_of = lambda degree, order: degree * degree + degree + order
    rows_of = lambda component: pl.ds(component * channels, channels)
    gather = lambda order: jnp.concatenate(
        [
            kept_ref[b, component_of(degree, order)].reshape(channels, lanes)
            for degree in range(abs(order), DEGREES)
        ],
        axis=0,
    )
    central = jnp.dot(weight_refs[0][...], gather(0), preferred_element_type=jnp.float32)
    gate = 1.0 / (1.0 + jnp.exp(-central[:channels]))
    for degree in range(DEGREES):
        gated_ref[rows_of(component_of(degree, 0)), :] = (
            central[degree * channels : (degree + 1) * channels] * gate
        ).astype(jnp.bfloat16)
    for order in range(1, DEGREES):
        plus = gather(order)
        minus = gather(-order)
        if order in THREE:
            deep = plus.shape[0]
            product = lambda at, right: jnp.dot(
                weight_refs[order][:, at * deep : (at + 1) * deep],
                right,
                preferred_element_type=jnp.float32,
            )
            both = product(0, plus + minus)
        for side in range(2):
            if order in THREE:
                mixed = both - product(1, minus) if side == 0 else both + product(2, plus)
            else:
                pair = [plus, -minus] if side == 0 else [minus, plus]
                mixed = jnp.dot(
                    weight_refs[order][...],
                    jnp.concatenate(pair, axis=0),
                    preferred_element_type=jnp.float32,
                )
            for column, degree in enumerate(range(order, DEGREES)):
                component = component_of(degree, order if side == 0 else -order)
                gated_ref[rows_of(component), :] = (
                    mixed[column * channels : (column + 1) * channels] * gate
                ).astype(jnp.bfloat16)

    edge = iota((1, lanes), 1) + b * lanes
    home = edge // slots
    slot = edge - home * slots
    window = 8
    first = jnp.minimum((b * lanes) // slots, atoms - window)
    position = slot + slots * (home - first) - slots * iota((window, lanes), 0)
    count = column_ref[pl.ds(first, window), :]
    count = jnp.concatenate([count] * (lanes // channels), axis=1)
    live = jnp.where(
        (position >= 0) & (position.astype(jnp.float32) < count) & (position < slots), 1.0, 0.0
    )
    offset = 0
    for degree in range(DEGREES):
        size = 2 * degree + 1
        summed = None
        for q in range(size):
            left = jnp.concatenate(
                [
                    jnp.broadcast_to(frame_t[b, pl.ds(offset + q * size + p, 1), :], live.shape)
                    * live
                    for p in range(size)
                ],
                axis=0,
            ).astype(jnp.bfloat16)
            term = lax.dot_general(
                left,
                gated_ref[rows_of(degree * degree + q), :],
                ACROSS,
                preferred_element_type=jnp.float32,
            )
            summed = term if summed is None else summed + term
        for p in range(size):
            at = degree * degree + p
            total_ref[at, pl.ds(first, window), :] = (
                total_ref[at, pl.ds(first, window), :] + summed[p * window : (p + 1) * window]
            )
        offset += size * size


def run(features, frames, radial, neighbours, counts, coefficients, stacks, lanes, plan):
    shapes = [(int(np.prod(w.shape[1:-1])), w.shape[-1]) for w in stacks]
    wide = lax.axis_size("wide")
    narrow = lax.axis_size("narrow")
    stacks = [flat_rows(w) for w in stacks]
    staged = [(w.shape[0], w.shape[1] // narrow, w.shape[2]) for w in stacks]
    rows = sum(shape[1] * shape[2] // 128 for shape in staged)
    unit = 16 * wide
    rows = -(-rows // unit) * unit
    part = rows // wide
    chips = wide // 2
    components, atoms, channels = features.shape
    edges, entries = frames.shape
    blocks = edges // lanes
    padded = -(-entries // 16) * 16
    groups = 2
    height = channels // groups
    anywhere = pl.BlockSpec(memory_space=pl.ANY)
    vmem = pl.BlockSpec(memory_space=pltpu.VMEM)
    dma = lambda *n: pltpu.SemaphoreType.DMA(n)
    bf16 = lambda *shape: pltpu.VMEM(shape, jnp.bfloat16)
    widest = 2 * DEGREES - 1
    return pl.pallas_call(
        functools.partial(whole_kernel, (wide, narrow, len(stacks)), shapes, plan),
        in_specs=[pl.BlockSpec(memory_space=pltpu.SMEM), vmem, vmem]
        + [anywhere] * (3 + len(stacks)),
        out_specs=vmem,
        out_shape=jax.ShapeDtypeStruct((components, atoms, channels), jnp.float32),
        scratch_shapes=[bf16(*shape) for shape in staged]
        + [bf16(n, k // 2 * 3 if at in THREE else k) for at, (k, n) in enumerate(shapes)]
        + [
            bf16(rows, 128),
            bf16(chips - 1, part, 128),
            bf16(chips * part, 128),
            bf16(chips - 1, part, 128),
            bf16(part, 128),
            bf16(components, 3 * atoms, channels),
            bf16(components, groups, height, 3 * atoms),
            bf16(edges, entries),
            bf16(edges, channels),
            bf16(neighbours.shape[0], atoms),
            bf16(blocks, 3 * atoms, lanes),
            pltpu.VMEM((blocks, padded, lanes), jnp.float32),
            bf16(blocks, groups, height, lanes),
            bf16(widest, groups, height, lanes),
            bf16(widest, groups, height, lanes),
            bf16(blocks, components, groups, height, lanes),
            bf16(narrow, wide * part, 128),
            bf16(components * channels, lanes),
            pltpu.VMEM((components, atoms, channels), jnp.float32),
            pltpu.VMEM((atoms, channels), jnp.float32),
            dma(len(stacks)),
            dma(3),
            dma(2 * DEGREES),
            dma(2 * DEGREES),
            dma(chips),
            dma(chips),
            dma(narrow - 1),
            dma(narrow - 1),
            dma(narrow * (chips - 1)),
            dma(narrow * (chips - 1)),
            dma(narrow * 2),
            dma(narrow * 2),
            dma(narrow * chips),
            dma(narrow * chips),
            pltpu.SemaphoreType.DMA,
        ],
        compiler_params=pltpu.CompilerParams(
            collective_id=0, has_side_effects=True, vmem_limit_bytes=60 * 1024 * 1024
        ),
    )(coefficients, neighbours, counts, features, frames, radial, *stacks)


def body(
    node_features,
    frames,
    radial,
    neighbours,
    counts,
    coefficients,
    w_zero,
    w_one,
    w_two,
    w_three,
    w_four,
):
    atoms, components, channels = node_features.shape
    slots = neighbours.shape[1]
    entries = frames.shape[2]
    edges = atoms * slots
    stacks = (w_zero, w_one, w_two, w_three, w_four)
    lanes = 256
    features = node_features.transpose(1, 0, 2)
    frames = frames.reshape(edges, entries)
    out = run(
        features,
        frames,
        radial.reshape(edges, channels),
        neighbours.T,
        counts.reshape(1, atoms),
        coefficients,
        stacks,
        lanes,
        PLAN,
    )
    return out.transpose(1, 0, 2)


def solution(mesh):
    spread = lambda rest: P(AXES, *([None] * rest))
    in_specs = (
        spread(2),
        spread(2),
        spread(2),
        spread(1),
        spread(0),
        P("wide"),
        P("wide", None, None),
        P("wide", None, None, None),
        P("wide", None, None, None),
        P("wide", None, None, None),
        P("wide", None, None, None),
    )
    return jax.shard_map(body, mesh=mesh, in_specs=in_specs, out_specs=spread(2), check_vma=False)
```

```python
import functools

import jax
import jax.numpy as jnp
import numpy as np
from jax import lax
from jax.experimental import pallas as pl
from jax.experimental.pallas import tpu as pltpu
from jax.sharding import PartitionSpec as P

DEGREES = 5
COMPONENTS = DEGREES * DEGREES
AXES = ("wide", "narrow")
THREE = (1, 3)
MESH = pl.DeviceIdType.MESH
EARLY = 2
PLAN = (8, 10, 18, 22, 24, 28, 34, 38, 42, 48, 54)


def flat_rows(weights):
    return weights.reshape(weights.shape[0], -1, weights.shape[-1])


def remote(src, dst, send, recv, device):
    return pltpu.make_async_remote_copy(
        src_ref=src,
        dst_ref=dst,
        send_sem=send,
        recv_sem=recv,
        device_id=device,
        device_id_type=MESH,
    )


def spans():
    return [(degree, degree * degree, 2 * degree + 1) for degree in reversed(range(DEGREES))]


def iota(shape, axis):
    return lax.broadcasted_iota(jnp.int32, shape, axis)


def eye(rows, columns):
    return (iota((rows, columns), 0) == iota((rows, columns), 1)).astype(jnp.bfloat16)


ACROSS = (((1,), (1,)), ((), ()))


def whole_kernel(sizes, shapes, plan, coefficient_ref, neighbours_ref, counts_ref, *refs):
    wide, narrow, count = sizes
    features_ref, frames_ref, radial_ref = refs[:3]
    refs = refs[3:]
    stacks = refs[:count]
    out_ref = refs[count]
    staged = refs[count + 1 : 2 * count + 1]
    weight_refs = refs[2 * count + 1 : 3 * count + 1]
    (
        partial_ref,
        received_ref,
        paired_ref,
        chip_ref,
        share_ref,
        extended_ref,
        upright_ref,
        frames_v,
        radial_v,
        rows_ref,
        picked_ref,
        frame_t,
        radial_t,
        source_ref,
        source_b,
        kept_ref,
        merged_ref,
        gated_ref,
        gated_b,
        total_ref,
        column_ref,
        load_sem,
        own_sem,
        halo_send,
        halo_recv,
        send_sem,
        recv_sem,
        line_send,
        line_recv,
        plane_send,
        plane_recv,
        cross_send,
        cross_recv,
        pair_send,
        pair_recv,
        local_sem,
    ) = refs[3 * count + 1 :]
    my_wide = lax.axis_index("wide")
    my_narrow = lax.axis_index("narrow")
    part = partial_ref.shape[0] // wide
    chips = wide // 2
    my_chip = my_wide // 2
    my_core = lax.rem(my_wide, 2)
    slots, atoms = neighbours_ref.shape
    blocks, _, lanes = picked_ref.shape
    entries = frames_v.shape[1]
    channels = radial_v.shape[1]
    extended = extended_ref.shape[1]

    loads = []
    for at, (stack, stage) in enumerate(zip(stacks, staged)):
        rows = stage.shape[1]
        loads.append(
            pltpu.make_async_copy(
                stack.at[:, pl.ds(pl.multiple_of(my_narrow * rows, 16), rows), :],
                stage,
                load_sem.at[at],
            )
        )
        loads[-1].start()
    own = [
        pltpu.make_async_copy(features_ref, extended_ref.at[:, pl.ds(atoms, atoms), :], own_sem.at[0]),
        pltpu.make_async_copy(frames_ref, frames_v, own_sem.at[1]),
        pltpu.make_async_copy(radial_ref, radial_v, own_sem.at[2]),
    ]
    for copy in own:
        copy.start()

    total = wide * narrow
    me = my_wide * narrow + my_narrow
    after = lax.rem(me + 1, total)
    before = lax.rem(me + total - 1, total)
    place = lambda flat: (flat // narrow, lax.rem(flat, narrow))
    partner = (my_wide + 1 - 2 * my_core, my_narrow)
    peers = [
        (lax.rem(my_chip + hop, chips) * 2 + my_core, my_narrow) for hop in range(1, chips)
    ] + [partner]
    line = [(my_wide, lax.rem(my_narrow + hop, narrow)) for hop in range(1, narrow)]
    greeted = [place(after), place(before)] + peers + line
    barrier = pltpu.get_barrier_semaphore()
    for device in greeted:
        pl.semaphore_signal(barrier, inc=1, device_id=device, device_id_type=MESH)
    pl.semaphore_wait(barrier, len(greeted))

    def halo_copy(at, side):
        degree, base, size = spans()[at]
        return remote(
            features_ref.at[pl.ds(base, size)],
            extended_ref.at[pl.ds(base, size), pl.ds(2 * side * atoms, atoms), :],
            halo_send.at[2 * at + side],
            halo_recv.at[2 * at + side],
            [place(after), place(before)][side],
        )

    for at in range(EARLY):
        for side in range(2):
            halo_copy(at, side).start()

    offset = 0
    for load, stage in zip(loads, staged):
        load.wait()
        experts, rows, columns = stage.shape
        for block in range(columns // 128):
            lane = pl.ds(block * 128, 128)
            value = coefficient_ref[0] * stage[0, :, lane].astype(jnp.float32)
            for expert in range(1, experts):
                value = value + coefficient_ref[expert] * stage[expert, :, lane].astype(
                    jnp.float32
                )
            partial_ref[pl.ds(offset, rows), :] = value.astype(jnp.bfloat16)
            offset += rows
    if offset < partial_ref.shape[0]:
        rest = partial_ref.shape[0] - offset
        partial_ref[pl.ds(offset, rest), :] = jnp.zeros((rest, 128), jnp.bfloat16)

    half = chips * part
    theirs = pl.ds(pl.multiple_of((1 - my_core) * half, 16), half)
    pairing = remote(
        partial_ref.at[theirs, :], paired_ref, send_sem.at[0], recv_sem.at[0], partner
    )
    pairing.start()

    everything = atoms * total
    relative = neighbours_ref[...] - (me * atoms - atoms)
    relative = jnp.where(relative < 0, relative + everything, relative)
    relative = jnp.where(relative >= everything, relative - everything, relative)
    relative = jnp.minimum(relative, 255)
    rows_ref[...] = relative.astype(jnp.float32).astype(jnp.bfloat16)
    for copy in own:
        copy.wait()

    def prepare(b, carried):
        edge = iota((1, lanes), 1) + b * lanes
        home = edge // slots
        slot = edge - home * slots
        chosen = (iota((atoms, lanes), 0) == home).astype(jnp.bfloat16)
        spread = jnp.dot(rows_ref[...], chosen, preferred_element_type=jnp.float32)
        index = jnp.sum(
            jnp.where(iota((slots, lanes), 0) == slot, spread, 0.0), axis=0, keepdims=True
        ).astype(jnp.int32)
        picked_ref[b] = (iota((extended, lanes), 0) == index).astype(jnp.bfloat16)
        row = pl.ds(pl.multiple_of(b * lanes, lanes), lanes)
        frame_t[b] = lax.dot_general(
            eye(frame_t.shape[1], entries),
            frames_v[row, :],
            ACROSS,
            preferred_element_type=jnp.float32,
        )
        scales = lax.dot_general(
            eye(channels, channels), radial_v[row, :], ACROSS, preferred_element_type=jnp.float32
        ).astype(jnp.bfloat16)
        radial_t[b] = scales.reshape(radial_t.shape[1:])
        return carried

    lax.fori_loop(0, blocks // 4, prepare, 0)

    pairing.wait_recv()
    scatter = []
    for hop in range(1, chips):
        target = lax.rem(my_chip + hop, chips)
        mine = pl.ds(pl.multiple_of(my_core * half + target * part, 16), part)
        there = pl.ds(pl.multiple_of(target * part, 16), part)
        chip_ref[hop - 1] = (
            partial_ref[mine, :].astype(jnp.float32) + paired_ref[there, :].astype(jnp.float32)
        ).astype(jnp.bfloat16)
        scatter.append(
            remote(
                chip_ref.at[hop - 1],
                received_ref.at[hop - 1],
                send_sem.at[hop],
                recv_sem.at[hop],
                (target * 2 + my_core, my_narrow),
            )
        )
        scatter[-1].start()
    lax.fori_loop(blocks // 4, blocks, prepare, 0)
    mine = pl.ds(pl.multiple_of(my_core * half + my_chip * part, 16), part)
    there = pl.ds(pl.multiple_of(my_chip * part, 16), part)
    summed = partial_ref[mine, :].astype(jnp.float32) + paired_ref[there, :].astype(jnp.float32)
    for hop in range(chips - 1):
        scatter[hop].wait_recv()
        summed = summed + received_ref[hop].astype(jnp.float32)
    share_ref[...] = summed.astype(jnp.bfloat16)

    my_place = my_core * chips + my_chip
    keep = pltpu.make_async_copy(share_ref, merged_ref.at[my_narrow, pl.ds(pl.multiple_of(my_place * part, 16), part), :], local_sem)
    keep.start()
    origin = lambda hop: lax.rem(my_narrow + narrow - hop, narrow)

    square = chips == 4
    if square:
        hops = [my_chip + 1 - 2 * lax.rem(my_chip, 2), my_chip + 2 - 4 * (my_chip // 2)]
        far = lax.rem(my_chip + 1, 2) + 2 * (1 - my_chip // 2)
        sources = hops
        owners = [my_chip] + hops + [far]
    else:
        hops = [lax.rem(my_chip + step, chips) for step in range(1, chips)]
        sources = [lax.rem(my_chip + chips - step, chips) for step in range(1, chips)]
        owners = [my_chip] + sources

    def spot(hop, chip, start=0, rows=part):
        row = (my_core * chips + chip) * part + start
        return merged_ref.at[origin(hop), pl.ds(pl.multiple_of(row, 16), rows), :]


    def line_copy(hop):
        return remote(
            share_ref,
            merged_ref.at[my_narrow, pl.ds(pl.multiple_of(my_place * part, 16), part), :],
            line_send.at[hop - 1],
            line_recv.at[hop - 1],
            line[hop - 1],
        )

    def plane_copy(hop, way):
        slot = spot(hop, my_chip)
        at = hop * len(hops) + way
        return remote(
            share_ref if hop == 0 else slot,
            slot,
            plane_send.at[at],
            plane_recv.at[at],
            (hops[way] * 2 + my_core, my_narrow),
        )

    def cross_copy(hop, way):
        slot = spot(hop, hops[way], way * cut, cut if way == 0 else part - cut)
        at = hop * 2 + way
        return remote(
            slot,
            slot,
            cross_send.at[at],
            cross_recv.at[at],
            (hops[1 - way] * 2 + my_core, my_narrow),
        )

    cut = part // 32 * 16

    def crossed(hop, way):
        slot = spot(hop, far, way * cut, cut if way == 0 else part - cut)
        at = hop * 2 + way
        return remote(
            slot,
            slot,
            cross_send.at[at],
            cross_recv.at[at],
            (hops[1 - way] * 2 + my_core, my_narrow),
        )

    def pair_copy(hop, step):
        slot = spot(hop, owners[step])
        at = hop * chips + step
        source = share_ref if hop == 0 and step == 0 else slot
        return remote(source, slot, pair_send.at[at], pair_recv.at[at], partner)

    def forward(hop):
        if hop:
            line_copy(hop).wait_recv()
        for way in range(len(hops)):
            plane_copy(hop, way).start()
        pair_copy(hop, 0).start()

    def relay(hop):
        for way in range(len(hops)):
            plane_copy(hop, way).wait_recv()
            if square:
                cross_copy(hop, way).start()
            pair_copy(hop, way + 1).start()

    def close(hop):
        for way in range(2):
            crossed(hop, way).wait_recv()
        pair_copy(hop, 3).start()

    for hop in range(1, narrow):
        line_copy(hop).start()
    for at in range(EARLY, DEGREES):
        for side in range(2):
            halo_copy(at, side).start()
    forward(0)

    steps = []
    for turn in range(narrow + 2):
        if 0 < turn < narrow:
            steps.append(functools.partial(forward, turn))
        if 0 < turn <= narrow:
            steps.append(functools.partial(relay, turn - 1))
        if square and turn > 1:
            steps.append(functools.partial(close, turn - 2))
    ticks = dict(zip(plan, steps))
    rest = steps[len(plan) :]

    groups, height = radial_t.shape[1:3]
    for at, (degree, base, size) in enumerate(spans()):
        for side in range(2):
            halo_copy(at, side).wait_recv()
        for component in range(base, base + size):
            upright_ref[component] = jnp.transpose(extended_ref[component]).reshape(
                upright_ref.shape[1:]
            )
        first = sum((2 * d + 1) ** 2 for d in range(degree))

        def fetch(b, group, source):
            left = jnp.concatenate(
                [upright_ref[base + q, group] for q in range(size)], axis=0
            )
            got = jnp.dot(left, picked_ref[b], preferred_element_type=jnp.float32)
            for q in range(size):
                source[q, group] = got[q * height : (q + 1) * height].astype(jnp.bfloat16)

        def rotate(b, group, source):
            for lane in range(0, lanes, 128):
                part_of = pl.ds(lane, 128)

                def entry(k):
                    row = frame_t[b, pl.ds(first + k, 1), part_of]
                    row = jnp.broadcast_to(row, (16, 128)).astype(jnp.bfloat16)
                    return jnp.concatenate([row] * (height // 16), axis=0)

                scale = radial_t[b, group, :, part_of]
                xs = [source[q, group, :, part_of] for q in range(size)]
                for p in range(size):
                    value = entry(p * size) * xs[0]
                    for q in range(1, size):
                        value = value + entry(p * size + q) * xs[q]
                    kept_ref[b, base + p, group, :, part_of] = value * scale

        def all_groups(work):
            if size > 5:
                lax.fori_loop(0, groups, lambda group, carried: (work(group), carried)[1], 0)
            else:
                for group in range(groups):
                    work(group)

        buffers = [source_ref, source_b]
        all_groups(lambda group: fetch(0, group, buffers[0]))

        def pair(i, carried):
            for block, step in ticks.items():
                if block // blocks == at:
                    pl.when(i == block % blocks // 2)(step)
            for k in range(2):
                b = 2 * i + k
                following = jnp.minimum(b + 1, blocks - 1)

                def both(group, b=b, following=following, k=k):
                    fetch(following, group, buffers[1 - k])
                    rotate(b, group, buffers[k])

                all_groups(both)
            return carried

        lax.fori_loop(0, blocks // 2, pair, 0)

    for step in rest:
        step()
    for hop in range(narrow):
        for step in range(chips):
            pair_copy(hop, step).wait_recv()
    for hop in range(1, narrow):
        line_copy(hop).wait_send()
    for hop in range(narrow):
        for step in range(chips):
            pair_copy(hop, step).wait_send()
        for way in range(len(hops)):
            plane_copy(hop, way).wait_send()
            if square:
                cross_copy(hop, way).wait_send()
    for copy in scatter + [pairing]:
        copy.wait_send()
    for at in range(DEGREES):
        for side in range(2):
            halo_copy(at, side).wait_send()
    keep.wait()

    offset = 0
    for order, (weight_ref, (rows, columns)) in enumerate(zip(weight_refs, shapes)):
        piece = rows // narrow
        for block in range(columns // 128):
            gathered = jnp.concatenate(
                [merged_ref[m, pl.ds(offset, piece), :] for m in range(narrow)], axis=0
            )
            if order in THREE:
                real = gathered[: rows // 2].astype(jnp.float32)
                imag = gathered[rows // 2 :].astype(jnp.float32)
                gathered = jnp.concatenate([real, real + imag, imag - real], axis=0).astype(
                    jnp.bfloat16
                )
            weight_ref[pl.ds(block * 128, 128), :] = jnp.transpose(gathered)
            offset += piece
    total_ref[...] = jnp.zeros_like(total_ref)
    square = (atoms, atoms)
    diagonal = iota(square, 0) == iota(square, 1)
    count = jnp.sum(
        jnp.where(diagonal, counts_ref[...].astype(jnp.float32), 0.0), axis=1, keepdims=True
    )
    column_ref[...] = jnp.broadcast_to(count, column_ref.shape)

    def mix(b, buffer, beside=lambda: None):
        mix_block(b, kept_ref, weight_refs, buffer, beside)

    def gather(b, buffer):
        sum_block(b, slots, frame_t, buffer, total_ref, column_ref)

    def two(i, carried):
        mix(2 * i + 1, gated_b, lambda: gather(2 * i, gated_ref))
        mix(2 * i + 2, gated_ref, lambda: gather(2 * i + 1, gated_b))
        return carried

    mix(0, gated_ref)
    lax.fori_loop(0, blocks // 2 - 1, two, 0)
    mix(blocks - 1, gated_b, lambda: gather(blocks - 2, gated_ref))
    gather(blocks - 1, gated_b)

    scale = 1.0 / jnp.sqrt(column_ref[...])
    for component in range(COMPONENTS):
        out_ref[component] = total_ref[component] * scale


def mix_block(b, kept_ref, weight_refs, gated_ref, beside):
    channels = gated_ref.shape[0] // COMPONENTS
    lanes = gated_ref.shape[1]
    component_of = lambda degree, order: degree * degree + degree + order
    rows_of = lambda component: pl.ds(component * channels, channels)
    gather = lambda order: jnp.concatenate(
        [
            kept_ref[b, component_of(degree, order)].reshape(channels, lanes)
            for degree in range(abs(order), DEGREES)
        ],
        axis=0,
    )
    central = jnp.dot(weight_refs[0][...], gather(0), preferred_element_type=jnp.float32)
    beside()
    gate = 1.0 / (1.0 + jnp.exp(-central[:channels]))
    for degree in range(DEGREES):
        gated_ref[rows_of(component_of(degree, 0)), :] = (
            central[degree * channels : (degree + 1) * channels] * gate
        ).astype(jnp.bfloat16)
    for order in range(1, DEGREES):
        plus = gather(order)
        minus = gather(-order)
        if order in THREE:
            deep = plus.shape[0]
            product = lambda at, right: jnp.dot(
                weight_refs[order][:, at * deep : (at + 1) * deep],
                right,
                preferred_element_type=jnp.float32,
            )
            both = product(0, plus + minus)
        for side in range(2):
            if order in THREE:
                mixed = both - product(1, minus) if side == 0 else both + product(2, plus)
            else:
                pair = [plus, -minus] if side == 0 else [minus, plus]
                mixed = jnp.dot(
                    weight_refs[order][...],
                    jnp.concatenate(pair, axis=0),
                    preferred_element_type=jnp.float32,
                )
            for column, degree in enumerate(range(order, DEGREES)):
                component = component_of(degree, order if side == 0 else -order)
                gated_ref[rows_of(component), :] = (
                    mixed[column * channels : (column + 1) * channels] * gate
                ).astype(jnp.bfloat16)


def sum_block(b, slots, frame_t, gated_ref, total_ref, column_ref):
    atoms, channels = column_ref.shape
    lanes = gated_ref.shape[1]
    rows_of = lambda component: pl.ds(component * channels, channels)
    edge = iota((1, lanes), 1) + b * lanes
    home = edge // slots
    slot = edge - home * slots
    window = 8
    first = jnp.minimum((b * lanes) // slots, atoms - window)
    position = slot + slots * (home - first) - slots * iota((window, lanes), 0)
    count = column_ref[pl.ds(first, window), :]
    count = jnp.concatenate([count] * (lanes // channels), axis=1)
    live = jnp.where(
        (position >= 0) & (position.astype(jnp.float32) < count) & (position < slots), 1.0, 0.0
    )
    offset = 0
    for degree in range(DEGREES):
        size = 2 * degree + 1
        summed = None
        for q in range(size):
            left = jnp.concatenate(
                [
                    jnp.broadcast_to(frame_t[b, pl.ds(offset + q * size + p, 1), :], live.shape)
                    * live
                    for p in range(size)
                ],
                axis=0,
            ).astype(jnp.bfloat16)
            term = lax.dot_general(
                left,
                gated_ref[rows_of(degree * degree + q), :],
                ACROSS,
                preferred_element_type=jnp.float32,
            )
            summed = term if summed is None else summed + term
        for p in range(size):
            at = degree * degree + p
            total_ref[at, pl.ds(first, window), :] = (
                total_ref[at, pl.ds(first, window), :] + summed[p * window : (p + 1) * window]
            )
        offset += size * size


def run(features, frames, radial, neighbours, counts, coefficients, stacks, lanes, plan):
    shapes = [(int(np.prod(w.shape[1:-1])), w.shape[-1]) for w in stacks]
    wide = lax.axis_size("wide")
    narrow = lax.axis_size("narrow")
    stacks = [flat_rows(w) for w in stacks]
    staged = [(w.shape[0], w.shape[1] // narrow, w.shape[2]) for w in stacks]
    rows = sum(shape[1] * shape[2] // 128 for shape in staged)
    unit = 16 * wide
    rows = -(-rows // unit) * unit
    part = rows // wide
    chips = wide // 2
    components, atoms, channels = features.shape
    edges, entries = frames.shape
    blocks = edges // lanes
    padded = -(-entries // 16) * 16
    groups = 2
    height = channels // groups
    anywhere = pl.BlockSpec(memory_space=pl.ANY)
    vmem = pl.BlockSpec(memory_space=pltpu.VMEM)
    dma = lambda *n: pltpu.SemaphoreType.DMA(n)
    bf16 = lambda *shape: pltpu.VMEM(shape, jnp.bfloat16)
    widest = 2 * DEGREES - 1
    return pl.pallas_call(
        functools.partial(whole_kernel, (wide, narrow, len(stacks)), shapes, plan),
        in_specs=[pl.BlockSpec(memory_space=pltpu.SMEM), vmem, vmem]
        + [anywhere] * (3 + len(stacks)),
        out_specs=vmem,
        out_shape=jax.ShapeDtypeStruct((components, atoms, channels), jnp.float32),
        scratch_shapes=[bf16(*shape) for shape in staged]
        + [bf16(n, k // 2 * 3 if at in THREE else k) for at, (k, n) in enumerate(shapes)]
        + [
            bf16(rows, 128),
            bf16(chips - 1, part, 128),
            bf16(chips * part, 128),
            bf16(chips - 1, part, 128),
            bf16(part, 128),
            bf16(components, 3 * atoms, channels),
            bf16(components, groups, height, 3 * atoms),
            bf16(edges, entries),
            bf16(edges, channels),
            bf16(neighbours.shape[0], atoms),
            bf16(blocks, 3 * atoms, lanes),
            pltpu.VMEM((blocks, padded, lanes), jnp.float32),
            bf16(blocks, groups, height, lanes),
            bf16(widest, groups, height, lanes),
            bf16(widest, groups, height, lanes),
            bf16(blocks, components, groups, height, lanes),
            bf16(narrow, wide * part, 128),
            bf16(components * channels, lanes),
            bf16(components * channels, lanes),
            pltpu.VMEM((components, atoms, channels), jnp.float32),
            pltpu.VMEM((atoms, channels), jnp.float32),
            dma(len(stacks)),
            dma(3),
            dma(2 * DEGREES),
            dma(2 * DEGREES),
            dma(chips),
            dma(chips),
            dma(narrow - 1),
            dma(narrow - 1),
            dma(narrow * (chips - 1)),
            dma(narrow * (chips - 1)),
            dma(narrow * 2),
            dma(narrow * 2),
            dma(narrow * chips),
            dma(narrow * chips),
            pltpu.SemaphoreType.DMA,
        ],
        compiler_params=pltpu.CompilerParams(
            collective_id=0, has_side_effects=True, vmem_limit_bytes=60 * 1024 * 1024
        ),
    )(coefficients, neighbours, counts, features, frames, radial, *stacks)


def body(
    node_features,
    frames,
    radial,
    neighbours,
    counts,
    coefficients,
    w_zero,
    w_one,
    w_two,
    w_three,
    w_four,
):
    atoms, components, channels = node_features.shape
    slots = neighbours.shape[1]
    entries = frames.shape[2]
    edges = atoms * slots
    stacks = (w_zero, w_one, w_two, w_three, w_four)
    lanes = 256
    features = node_features.transpose(1, 0, 2)
    frames = frames.reshape(edges, entries)
    out = run(
        features,
        frames,
        radial.reshape(edges, channels),
        neighbours.T,
        counts.reshape(1, atoms),
        coefficients,
        stacks,
        lanes,
        PLAN,
    )
    return out.transpose(1, 0, 2)


def solution(mesh):
    spread = lambda rest: P(AXES, *([None] * rest))
    in_specs = (
        spread(2),
        spread(2),
        spread(2),
        spread(1),
        spread(0),
        P("wide"),
        P("wide", None, None),
        P("wide", None, None, None),
        P("wide", None, None, None),
        P("wide", None, None, None),
        P("wide", None, None, None),
    )
    return jax.shard_map(body, mesh=mesh, in_specs=in_specs, out_specs=spread(2), check_vma=False)
```

```python
import functools

import jax
import jax.numpy as jnp
import numpy as np
from jax import lax
from jax.experimental import pallas as pl
from jax.experimental.pallas import tpu as pltpu
from jax.sharding import PartitionSpec as P

DEGREES = 5
COMPONENTS = DEGREES * DEGREES
AXES = ("wide", "narrow")
THREE = (1, 2, 3)
MESH = pl.DeviceIdType.MESH
EARLY = 2
PLAN = (8, 10, 18, 22, 24, 28, 34, 38, 42, 48, 54)


def flat_rows(weights):
    return weights.reshape(weights.shape[0], -1, weights.shape[-1])


def remote(src, dst, send, recv, device):
    return pltpu.make_async_remote_copy(
        src_ref=src,
        dst_ref=dst,
        send_sem=send,
        recv_sem=recv,
        device_id=device,
        device_id_type=MESH,
    )


def spans():
    return [(degree, degree * degree, 2 * degree + 1) for degree in reversed(range(DEGREES))]


def iota(shape, axis):
    return lax.broadcasted_iota(jnp.int32, shape, axis)


def eye(rows, columns):
    return (iota((rows, columns), 0) == iota((rows, columns), 1)).astype(jnp.bfloat16)


ACROSS = (((1,), (1,)), ((), ()))


def whole_kernel(sizes, shapes, plan, coefficient_ref, neighbours_ref, counts_ref, *refs):
    wide, narrow, count = sizes
    features_ref, frames_ref, radial_ref = refs[:3]
    refs = refs[3:]
    stacks = refs[:count]
    out_ref = refs[count]
    staged = refs[count + 1 : 2 * count + 1]
    weight_refs = refs[2 * count + 1 : 3 * count + 1]
    (
        partial_ref,
        received_ref,
        paired_ref,
        chip_ref,
        share_ref,
        extended_ref,
        upright_ref,
        frames_v,
        radial_v,
        rows_ref,
        picked_ref,
        frame_t,
        radial_t,
        source_ref,
        source_b,
        kept_ref,
        merged_ref,
        gated_ref,
        gated_b,
        total_ref,
        column_ref,
        load_sem,
        own_sem,
        halo_send,
        halo_recv,
        send_sem,
        recv_sem,
        line_send,
        line_recv,
        plane_send,
        plane_recv,
        cross_send,
        cross_recv,
        pair_send,
        pair_recv,
        local_sem,
    ) = refs[3 * count + 1 :]
    my_wide = lax.axis_index("wide")
    my_narrow = lax.axis_index("narrow")
    part = partial_ref.shape[0] // wide
    chips = wide // 2
    my_chip = my_wide // 2
    my_core = lax.rem(my_wide, 2)
    slots, atoms = neighbours_ref.shape
    blocks, _, lanes = picked_ref.shape
    entries = frames_v.shape[1]
    channels = radial_v.shape[1]
    extended = extended_ref.shape[1]

    loads = []
    for at, (stack, stage) in enumerate(zip(stacks, staged)):
        rows = stage.shape[1]
        loads.append(
            pltpu.make_async_copy(
                stack.at[:, pl.ds(pl.multiple_of(my_narrow * rows, 16), rows), :],
                stage,
                load_sem.at[at],
            )
        )
        loads[-1].start()
    own = [
        pltpu.make_async_copy(features_ref, extended_ref.at[:, pl.ds(atoms, atoms), :], own_sem.at[0]),
        pltpu.make_async_copy(frames_ref, frames_v, own_sem.at[1]),
        pltpu.make_async_copy(radial_ref, radial_v, own_sem.at[2]),
    ]
    for copy in own:
        copy.start()

    total = wide * narrow
    me = my_wide * narrow + my_narrow
    after = lax.rem(me + 1, total)
    before = lax.rem(me + total - 1, total)
    place = lambda flat: (flat // narrow, lax.rem(flat, narrow))
    partner = (my_wide + 1 - 2 * my_core, my_narrow)
    peers = [
        (lax.rem(my_chip + hop, chips) * 2 + my_core, my_narrow) for hop in range(1, chips)
    ] + [partner]
    line = [(my_wide, lax.rem(my_narrow + hop, narrow)) for hop in range(1, narrow)]
    greeted = [place(after), place(before)] + peers + line
    barrier = pltpu.get_barrier_semaphore()
    for device in greeted:
        pl.semaphore_signal(barrier, inc=1, device_id=device, device_id_type=MESH)
    pl.semaphore_wait(barrier, len(greeted))

    def halo_copy(at, side):
        degree, base, size = spans()[at]
        return remote(
            features_ref.at[pl.ds(base, size)],
            extended_ref.at[pl.ds(base, size), pl.ds(2 * side * atoms, atoms), :],
            halo_send.at[2 * at + side],
            halo_recv.at[2 * at + side],
            [place(after), place(before)][side],
        )

    for at in range(EARLY):
        for side in range(2):
            halo_copy(at, side).start()

    offset = 0
    for load, stage in zip(loads, staged):
        load.wait()
        experts, rows, columns = stage.shape
        for block in range(columns // 128):
            lane = pl.ds(block * 128, 128)
            value = coefficient_ref[0] * stage[0, :, lane].astype(jnp.float32)
            for expert in range(1, experts):
                value = value + coefficient_ref[expert] * stage[expert, :, lane].astype(
                    jnp.float32
                )
            partial_ref[pl.ds(offset, rows), :] = value.astype(jnp.bfloat16)
            offset += rows
    if offset < partial_ref.shape[0]:
        rest = partial_ref.shape[0] - offset
        partial_ref[pl.ds(offset, rest), :] = jnp.zeros((rest, 128), jnp.bfloat16)

    half = chips * part
    theirs = pl.ds(pl.multiple_of((1 - my_core) * half, 16), half)
    pairing = remote(
        partial_ref.at[theirs, :], paired_ref, send_sem.at[0], recv_sem.at[0], partner
    )
    pairing.start()

    everything = atoms * total
    relative = neighbours_ref[...] - (me * atoms - atoms)
    relative = jnp.where(relative < 0, relative + everything, relative)
    relative = jnp.where(relative >= everything, relative - everything, relative)
    relative = jnp.minimum(relative, 255)
    rows_ref[...] = relative.astype(jnp.float32).astype(jnp.bfloat16)
    for copy in own:
        copy.wait()

    def prepare(b, carried):
        edge = iota((1, lanes), 1) + b * lanes
        home = edge // slots
        slot = edge - home * slots
        chosen = (iota((atoms, lanes), 0) == home).astype(jnp.bfloat16)
        spread = jnp.dot(rows_ref[...], chosen, preferred_element_type=jnp.float32)
        index = jnp.sum(
            jnp.where(iota((slots, lanes), 0) == slot, spread, 0.0), axis=0, keepdims=True
        ).astype(jnp.int32)
        picked_ref[b] = (iota((extended, lanes), 0) == index).astype(jnp.bfloat16)
        row = pl.ds(pl.multiple_of(b * lanes, lanes), lanes)
        frame_t[b] = lax.dot_general(
            eye(frame_t.shape[1], entries),
            frames_v[row, :],
            ACROSS,
            preferred_element_type=jnp.float32,
        )
        scales = lax.dot_general(
            eye(channels, channels), radial_v[row, :], ACROSS, preferred_element_type=jnp.float32
        ).astype(jnp.bfloat16)
        radial_t[b] = scales.reshape(radial_t.shape[1:])
        return carried

    lax.fori_loop(0, blocks // 4, prepare, 0)

    pairing.wait_recv()
    scatter = []
    for hop in range(1, chips):
        target = lax.rem(my_chip + hop, chips)
        mine = pl.ds(pl.multiple_of(my_core * half + target * part, 16), part)
        there = pl.ds(pl.multiple_of(target * part, 16), part)
        chip_ref[hop - 1] = (
            partial_ref[mine, :].astype(jnp.float32) + paired_ref[there, :].astype(jnp.float32)
        ).astype(jnp.bfloat16)
        scatter.append(
            remote(
                chip_ref.at[hop - 1],
                received_ref.at[hop - 1],
                send_sem.at[hop],
                recv_sem.at[hop],
                (target * 2 + my_core, my_narrow),
            )
        )
        scatter[-1].start()
    lax.fori_loop(blocks // 4, blocks, prepare, 0)
    mine = pl.ds(pl.multiple_of(my_core * half + my_chip * part, 16), part)
    there = pl.ds(pl.multiple_of(my_chip * part, 16), part)
    summed = partial_ref[mine, :].astype(jnp.float32) + paired_ref[there, :].astype(jnp.float32)
    for hop in range(chips - 1):
        scatter[hop].wait_recv()
        summed = summed + received_ref[hop].astype(jnp.float32)
    share_ref[...] = summed.astype(jnp.bfloat16)

    my_place = my_core * chips + my_chip
    keep = pltpu.make_async_copy(share_ref, merged_ref.at[my_narrow, pl.ds(pl.multiple_of(my_place * part, 16), part), :], local_sem)
    keep.start()
    origin = lambda hop: lax.rem(my_narrow + narrow - hop, narrow)

    square = chips == 4
    if square:
        hops = [my_chip + 1 - 2 * lax.rem(my_chip, 2), my_chip + 2 - 4 * (my_chip // 2)]
        far = lax.rem(my_chip + 1, 2) + 2 * (1 - my_chip // 2)
        sources = hops
        owners = [my_chip] + hops + [far]
    else:
        hops = [lax.rem(my_chip + step, chips) for step in range(1, chips)]
        sources = [lax.rem(my_chip + chips - step, chips) for step in range(1, chips)]
        owners = [my_chip] + sources

    def spot(hop, chip, start=0, rows=part):
        row = (my_core * chips + chip) * part + start
        return merged_ref.at[origin(hop), pl.ds(pl.multiple_of(row, 16), rows), :]


    def line_copy(hop):
        return remote(
            share_ref,
            merged_ref.at[my_narrow, pl.ds(pl.multiple_of(my_place * part, 16), part), :],
            line_send.at[hop - 1],
            line_recv.at[hop - 1],
            line[hop - 1],
        )

    def plane_copy(hop, way):
        slot = spot(hop, my_chip)
        at = hop * len(hops) + way
        return remote(
            share_ref if hop == 0 else slot,
            slot,
            plane_send.at[at],
            plane_recv.at[at],
            (hops[way] * 2 + my_core, my_narrow),
        )

    def cross_copy(hop, way):
        slot = spot(hop, hops[way], way * cut, cut if way == 0 else part - cut)
        at = hop * 2 + way
        return remote(
            slot,
            slot,
            cross_send.at[at],
            cross_recv.at[at],
            (hops[1 - way] * 2 + my_core, my_narrow),
        )

    cut = part // 32 * 16

    def crossed(hop, way):
        slot = spot(hop, far, way * cut, cut if way == 0 else part - cut)
        at = hop * 2 + way
        return remote(
            slot,
            slot,
            cross_send.at[at],
            cross_recv.at[at],
            (hops[1 - way] * 2 + my_core, my_narrow),
        )

    def pair_copy(hop, step):
        slot = spot(hop, owners[step])
        at = hop * chips + step
        source = share_ref if hop == 0 and step == 0 else slot
        return remote(source, slot, pair_send.at[at], pair_recv.at[at], partner)

    def forward(hop):
        if hop:
            line_copy(hop).wait_recv()
        for way in range(len(hops)):
            plane_copy(hop, way).start()
        pair_copy(hop, 0).start()

    def relay(hop):
        for way in range(len(hops)):
            plane_copy(hop, way).wait_recv()
            if square:
                cross_copy(hop, way).start()
            pair_copy(hop, way + 1).start()

    def close(hop):
        for way in range(2):
            crossed(hop, way).wait_recv()
        pair_copy(hop, 3).start()

    for hop in range(1, narrow):
        line_copy(hop).start()
    for at in range(EARLY, DEGREES):
        for side in range(2):
            halo_copy(at, side).start()
    forward(0)

    steps = []
    for turn in range(narrow + 2):
        if 0 < turn < narrow:
            steps.append(functools.partial(forward, turn))
        if 0 < turn <= narrow:
            steps.append(functools.partial(relay, turn - 1))
        if square and turn > 1:
            steps.append(functools.partial(close, turn - 2))
    ticks = dict(zip(plan, steps))
    rest = steps[len(plan) :]

    groups, height = radial_t.shape[1:3]
    for at, (degree, base, size) in enumerate(spans()):
        for side in range(2):
            halo_copy(at, side).wait_recv()
        for component in range(base, base + size):
            upright_ref[component] = jnp.transpose(extended_ref[component]).reshape(
                upright_ref.shape[1:]
            )
        first = sum((2 * d + 1) ** 2 for d in range(degree))

        def fetch(b, group, source):
            left = jnp.concatenate(
                [upright_ref[base + q, group] for q in range(size)], axis=0
            )
            got = jnp.dot(left, picked_ref[b], preferred_element_type=jnp.float32)
            for q in range(size):
                source[q, group] = got[q * height : (q + 1) * height].astype(jnp.bfloat16)

        def rotate(b, group, source):
            for lane in range(0, lanes, 128):
                part_of = pl.ds(lane, 128)

                def entry(k):
                    row = frame_t[b, pl.ds(first + k, 1), part_of]
                    row = jnp.broadcast_to(row, (16, 128)).astype(jnp.bfloat16)
                    return jnp.concatenate([row] * (height // 16), axis=0)

                scale = radial_t[b, group, :, part_of]
                xs = [source[q, group, :, part_of] for q in range(size)]
                for p in range(size):
                    value = entry(p * size) * xs[0]
                    for q in range(1, size):
                        value = value + entry(p * size + q) * xs[q]
                    kept_ref[b, base + p, group, :, part_of] = value * scale

        def all_groups(work):
            if size > 5:
                lax.fori_loop(0, groups, lambda group, carried: (work(group), carried)[1], 0)
            else:
                for group in range(groups):
                    work(group)

        buffers = [source_ref, source_b]
        all_groups(lambda group: fetch(0, group, buffers[0]))

        def pair(i, carried):
            for block, step in ticks.items():
                if block // blocks == at:
                    pl.when(i == block % blocks // 2)(step)
            for k in range(2):
                b = 2 * i + k
                following = jnp.minimum(b + 1, blocks - 1)

                def both(group, b=b, following=following, k=k):
                    fetch(following, group, buffers[1 - k])
                    rotate(b, group, buffers[k])

                all_groups(both)
            return carried

        lax.fori_loop(0, blocks // 2, pair, 0)

    for step in rest:
        step()
    for hop in range(narrow):
        for step in range(chips):
            pair_copy(hop, step).wait_recv()
    for hop in range(1, narrow):
        line_copy(hop).wait_send()
    for hop in range(narrow):
        for step in range(chips):
            pair_copy(hop, step).wait_send()
        for way in range(len(hops)):
            plane_copy(hop, way).wait_send()
            if square:
                cross_copy(hop, way).wait_send()
    for copy in scatter + [pairing]:
        copy.wait_send()
    for at in range(DEGREES):
        for side in range(2):
            halo_copy(at, side).wait_send()
    keep.wait()

    offset = 0
    for order, (weight_ref, (rows, columns)) in enumerate(zip(weight_refs, shapes)):
        piece = rows // narrow
        for block in range(columns // 128):
            gathered = jnp.concatenate(
                [merged_ref[m, pl.ds(offset, piece), :] for m in range(narrow)], axis=0
            )
            if order in THREE:
                real = gathered[: rows // 2].astype(jnp.float32)
                imag = gathered[rows // 2 :].astype(jnp.float32)
                gathered = jnp.concatenate([real, real + imag, imag - real], axis=0).astype(
                    jnp.bfloat16
                )
            weight_ref[pl.ds(block * 128, 128), :] = jnp.transpose(gathered)
            offset += piece
    total_ref[...] = jnp.zeros_like(total_ref)
    square = (atoms, atoms)
    diagonal = iota(square, 0) == iota(square, 1)
    count = jnp.sum(
        jnp.where(diagonal, counts_ref[...].astype(jnp.float32), 0.0), axis=1, keepdims=True
    )
    column_ref[...] = jnp.broadcast_to(count, column_ref.shape)

    def mix(b, buffer, beside=lambda: None):
        mix_block(b, kept_ref, weight_refs, buffer, beside)

    def gather(b, buffer):
        sum_block(b, slots, frame_t, buffer, total_ref, column_ref)

    def two(i, carried):
        mix(2 * i + 1, gated_b, lambda: gather(2 * i, gated_ref))
        mix(2 * i + 2, gated_ref, lambda: gather(2 * i + 1, gated_b))
        return carried

    mix(0, gated_ref)
    lax.fori_loop(0, blocks // 2 - 1, two, 0)
    mix(blocks - 1, gated_b, lambda: gather(blocks - 2, gated_ref))
    gather(blocks - 1, gated_b)

    scale = 1.0 / jnp.sqrt(column_ref[...])
    for component in range(COMPONENTS):
        out_ref[component] = total_ref[component] * scale


def mix_block(b, kept_ref, weight_refs, gated_ref, beside):
    channels = gated_ref.shape[0] // COMPONENTS
    lanes = gated_ref.shape[1]
    component_of = lambda degree, order: degree * degree + degree + order
    rows_of = lambda component: pl.ds(component * channels, channels)
    gather = lambda order: jnp.concatenate(
        [
            kept_ref[b, component_of(degree, order)].reshape(channels, lanes)
            for degree in range(abs(order), DEGREES)
        ],
        axis=0,
    )
    central = jnp.dot(weight_refs[0][...], gather(0), preferred_element_type=jnp.float32)
    beside()
    gate = 1.0 / (1.0 + jnp.exp(-central[:channels]))
    for degree in range(DEGREES):
        gated_ref[rows_of(component_of(degree, 0)), :] = (
            central[degree * channels : (degree + 1) * channels] * gate
        ).astype(jnp.bfloat16)
    for order in range(1, DEGREES):
        plus = gather(order)
        minus = gather(-order)
        if order in THREE:
            deep = plus.shape[0]
            full = deep // 256 * 256
            weight = weight_refs[order]
            product = lambda left, right: jnp.dot(left, right, preferred_element_type=jnp.float32)
            fully = lambda at, right: product(
                weight[:, at * deep : at * deep + full], right[:full]
            )
            left_of = lambda at: weight[:, at * deep + full : (at + 1) * deep]
            sums = plus + minus
            both = fully(0, sums)
        for side in range(2):
            if order in THREE:
                other = minus if side == 0 else plus
                term = fully(side + 1, other)
                mixed = both - term if side == 0 else both + term
                if full < deep:
                    tail = -other[full:] if side == 0 else other[full:]
                    mixed = mixed + product(
                        jnp.concatenate([left_of(0), left_of(side + 1)], axis=1),
                        jnp.concatenate([sums[full:], tail], axis=0),
                    )
            else:
                pair = [plus, -minus] if side == 0 else [minus, plus]
                mixed = jnp.dot(
                    weight_refs[order][...],
                    jnp.concatenate(pair, axis=0),
                    preferred_element_type=jnp.float32,
                )
            for column, degree in enumerate(range(order, DEGREES)):
                component = component_of(degree, order if side == 0 else -order)
                gated_ref[rows_of(component), :] = (
                    mixed[column * channels : (column + 1) * channels] * gate
                ).astype(jnp.bfloat16)


def sum_block(b, slots, frame_t, gated_ref, total_ref, column_ref):
    atoms, channels = column_ref.shape
    lanes = gated_ref.shape[1]
    rows_of = lambda component: pl.ds(component * channels, channels)
    edge = iota((1, lanes), 1) + b * lanes
    home = edge // slots
    slot = edge - home * slots
    window = 8
    first = jnp.minimum((b * lanes) // slots, atoms - window)
    position = slot + slots * (home - first) - slots * iota((window, lanes), 0)
    count = column_ref[pl.ds(first, window), :]
    count = jnp.concatenate([count] * (lanes // channels), axis=1)
    live = jnp.where(
        (position >= 0) & (position.astype(jnp.float32) < count) & (position < slots), 1.0, 0.0
    )
    offset = 0
    for degree in range(DEGREES):
        size = 2 * degree + 1
        summed = None
        for q in range(size):
            left = jnp.concatenate(
                [
                    jnp.broadcast_to(frame_t[b, pl.ds(offset + q * size + p, 1), :], live.shape)
                    * live
                    for p in range(size)
                ],
                axis=0,
            ).astype(jnp.bfloat16)
            term = lax.dot_general(
                left,
                gated_ref[rows_of(degree * degree + q), :],
                ACROSS,
                preferred_element_type=jnp.float32,
            )
            summed = term if summed is None else summed + term
        for p in range(size):
            at = degree * degree + p
            total_ref[at, pl.ds(first, window), :] = (
                total_ref[at, pl.ds(first, window), :] + summed[p * window : (p + 1) * window]
            )
        offset += size * size


def run(features, frames, radial, neighbours, counts, coefficients, stacks, lanes, plan):
    shapes = [(int(np.prod(w.shape[1:-1])), w.shape[-1]) for w in stacks]
    wide = lax.axis_size("wide")
    narrow = lax.axis_size("narrow")
    stacks = [flat_rows(w) for w in stacks]
    staged = [(w.shape[0], w.shape[1] // narrow, w.shape[2]) for w in stacks]
    rows = sum(shape[1] * shape[2] // 128 for shape in staged)
    unit = 16 * wide
    rows = -(-rows // unit) * unit
    part = rows // wide
    chips = wide // 2
    components, atoms, channels = features.shape
    edges, entries = frames.shape
    blocks = edges // lanes
    padded = -(-entries // 16) * 16
    groups = 2
    height = channels // groups
    anywhere = pl.BlockSpec(memory_space=pl.ANY)
    vmem = pl.BlockSpec(memory_space=pltpu.VMEM)
    dma = lambda *n: pltpu.SemaphoreType.DMA(n)
    bf16 = lambda *shape: pltpu.VMEM(shape, jnp.bfloat16)
    widest = 2 * DEGREES - 1
    return pl.pallas_call(
        functools.partial(whole_kernel, (wide, narrow, len(stacks)), shapes, plan),
        in_specs=[pl.BlockSpec(memory_space=pltpu.SMEM), vmem, vmem]
        + [anywhere] * (3 + len(stacks)),
        out_specs=vmem,
        out_shape=jax.ShapeDtypeStruct((components, atoms, channels), jnp.float32),
        scratch_shapes=[bf16(*shape) for shape in staged]
        + [bf16(n, k // 2 * 3 if at in THREE else k) for at, (k, n) in enumerate(shapes)]
        + [
            bf16(rows, 128),
            bf16(chips - 1, part, 128),
            bf16(chips * part, 128),
            bf16(chips - 1, part, 128),
            bf16(part, 128),
            bf16(components, 3 * atoms, channels),
            bf16(components, groups, height, 3 * atoms),
            bf16(edges, entries),
            bf16(edges, channels),
            bf16(neighbours.shape[0], atoms),
            bf16(blocks, 3 * atoms, lanes),
            pltpu.VMEM((blocks, padded, lanes), jnp.float32),
            bf16(blocks, groups, height, lanes),
            bf16(widest, groups, height, lanes),
            bf16(widest, groups, height, lanes),
            bf16(blocks, components, groups, height, lanes),
            bf16(narrow, wide * part, 128),
            bf16(components * channels, lanes),
            bf16(components * channels, lanes),
            pltpu.VMEM((components, atoms, channels), jnp.float32),
            pltpu.VMEM((atoms, channels), jnp.float32),
            dma(len(stacks)),
            dma(3),
            dma(2 * DEGREES),
            dma(2 * DEGREES),
            dma(chips),
            dma(chips),
            dma(narrow - 1),
            dma(narrow - 1),
            dma(narrow * (chips - 1)),
            dma(narrow * (chips - 1)),
            dma(narrow * 2),
            dma(narrow * 2),
            dma(narrow * chips),
            dma(narrow * chips),
            pltpu.SemaphoreType.DMA,
        ],
        compiler_params=pltpu.CompilerParams(
            collective_id=0, has_side_effects=True, vmem_limit_bytes=60 * 1024 * 1024
        ),
    )(coefficients, neighbours, counts, features, frames, radial, *stacks)


def body(
    node_features,
    frames,
    radial,
    neighbours,
    counts,
    coefficients,
    w_zero,
    w_one,
    w_two,
    w_three,
    w_four,
):
    atoms, components, channels = node_features.shape
    slots = neighbours.shape[1]
    entries = frames.shape[2]
    edges = atoms * slots
    stacks = (w_zero, w_one, w_two, w_three, w_four)
    lanes = 256
    features = node_features.transpose(1, 0, 2)
    frames = frames.reshape(edges, entries)
    out = run(
        features,
        frames,
        radial.reshape(edges, channels),
        neighbours.T,
        counts.reshape(1, atoms),
        coefficients,
        stacks,
        lanes,
        PLAN,
    )
    return out.transpose(1, 0, 2)


def solution(mesh):
    spread = lambda rest: P(AXES, *([None] * rest))
    in_specs = (
        spread(2),
        spread(2),
        spread(2),
        spread(1),
        spread(0),
        P("wide"),
        P("wide", None, None),
        P("wide", None, None, None),
        P("wide", None, None, None),
        P("wide", None, None, None),
        P("wide", None, None, None),
    )
    return jax.shard_map(body, mesh=mesh, in_specs=in_specs, out_specs=spread(2), check_vma=False)
```

```python
import functools

import jax
import jax.numpy as jnp
import numpy as np
from jax import lax
from jax.experimental import pallas as pl
from jax.experimental.pallas import tpu as pltpu
from jax.sharding import PartitionSpec as P

DEGREES = 5
COMPONENTS = DEGREES * DEGREES
AXES = ("wide", "narrow")
THREE = (1, 2, 3)
MESH = pl.DeviceIdType.MESH
EARLY = 2
PLAN = (8, 10, 18, 22, 24, 26, 32, 36, 40, 44, 48)


def flat_rows(weights):
    return weights.reshape(weights.shape[0], -1, weights.shape[-1])


def remote(src, dst, send, recv, device):
    return pltpu.make_async_remote_copy(
        src_ref=src,
        dst_ref=dst,
        send_sem=send,
        recv_sem=recv,
        device_id=device,
        device_id_type=MESH,
    )


def spans():
    return [(degree, degree * degree, 2 * degree + 1) for degree in reversed(range(DEGREES))]


def iota(shape, axis):
    return lax.broadcasted_iota(jnp.int32, shape, axis)


def eye(rows, columns):
    return (iota((rows, columns), 0) == iota((rows, columns), 1)).astype(jnp.bfloat16)


ACROSS = (((1,), (1,)), ((), ()))


def whole_kernel(sizes, shapes, plan, coefficient_ref, neighbours_ref, counts_ref, *refs):
    wide, narrow, count = sizes
    features_ref, frames_ref, radial_ref = refs[:3]
    refs = refs[3:]
    stacks = refs[:count]
    out_ref = refs[count]
    staged = refs[count + 1 : 2 * count + 1]
    weight_refs = refs[2 * count + 1 : 3 * count + 1]
    (
        partial_ref,
        received_ref,
        paired_ref,
        chip_ref,
        share_ref,
        extended_ref,
        upright_ref,
        frames_v,
        radial_v,
        rows_ref,
        picked_ref,
        frame_t,
        radial_t,
        source_ref,
        source_b,
        kept_ref,
        merged_ref,
        gated_ref,
        gated_b,
        total_ref,
        column_ref,
        load_sem,
        own_sem,
        halo_send,
        halo_recv,
        send_sem,
        recv_sem,
        line_send,
        line_recv,
        plane_send,
        plane_recv,
        cross_send,
        cross_recv,
        pair_send,
        pair_recv,
        local_sem,
    ) = refs[3 * count + 1 :]
    my_wide = lax.axis_index("wide")
    my_narrow = lax.axis_index("narrow")
    part = partial_ref.shape[0] // wide
    chips = wide // 2
    my_chip = my_wide // 2
    my_core = lax.rem(my_wide, 2)
    slots, atoms = neighbours_ref.shape
    blocks, _, lanes = picked_ref.shape
    entries = frames_v.shape[1]
    channels = radial_v.shape[1]
    extended = extended_ref.shape[1]

    loads = []
    for at, (stack, stage) in enumerate(zip(stacks, staged)):
        rows = stage.shape[1]
        loads.append(
            pltpu.make_async_copy(
                stack.at[:, pl.ds(pl.multiple_of(my_narrow * rows, 16), rows), :],
                stage,
                load_sem.at[at],
            )
        )
        loads[-1].start()
    own = [
        pltpu.make_async_copy(features_ref, extended_ref.at[:, pl.ds(atoms, atoms), :], own_sem.at[0]),
        pltpu.make_async_copy(frames_ref, frames_v, own_sem.at[1]),
        pltpu.make_async_copy(radial_ref, radial_v, own_sem.at[2]),
    ]
    for copy in own:
        copy.start()

    total = wide * narrow
    me = my_wide * narrow + my_narrow
    after = lax.rem(me + 1, total)
    before = lax.rem(me + total - 1, total)
    place = lambda flat: (flat // narrow, lax.rem(flat, narrow))
    partner = (my_wide + 1 - 2 * my_core, my_narrow)
    peers = [
        (lax.rem(my_chip + hop, chips) * 2 + my_core, my_narrow) for hop in range(1, chips)
    ] + [partner]
    line = [(my_wide, lax.rem(my_narrow + hop, narrow)) for hop in range(1, narrow)]
    greeted = [place(after), place(before)] + peers + line
    barrier = pltpu.get_barrier_semaphore()
    for device in greeted:
        pl.semaphore_signal(barrier, inc=1, device_id=device, device_id_type=MESH)
    pl.semaphore_wait(barrier, len(greeted))

    def halo_copy(at, side):
        degree, base, size = spans()[at]
        return remote(
            features_ref.at[pl.ds(base, size)],
            extended_ref.at[pl.ds(base, size), pl.ds(2 * side * atoms, atoms), :],
            halo_send.at[2 * at + side],
            halo_recv.at[2 * at + side],
            [place(after), place(before)][side],
        )

    for at in range(EARLY):
        for side in range(2):
            halo_copy(at, side).start()

    offset = 0
    for load, stage in zip(loads, staged):
        load.wait()
        experts, rows, columns = stage.shape
        for block in range(columns // 128):
            lane = pl.ds(block * 128, 128)
            value = coefficient_ref[0] * stage[0, :, lane].astype(jnp.float32)
            for expert in range(1, experts):
                value = value + coefficient_ref[expert] * stage[expert, :, lane].astype(
                    jnp.float32
                )
            partial_ref[pl.ds(offset, rows), :] = value.astype(jnp.bfloat16)
            offset += rows
    if offset < partial_ref.shape[0]:
        rest = partial_ref.shape[0] - offset
        partial_ref[pl.ds(offset, rest), :] = jnp.zeros((rest, 128), jnp.bfloat16)

    half = chips * part
    theirs = pl.ds(pl.multiple_of((1 - my_core) * half, 16), half)
    pairing = remote(
        partial_ref.at[theirs, :], paired_ref, send_sem.at[0], recv_sem.at[0], partner
    )
    pairing.start()

    everything = atoms * total
    relative = neighbours_ref[...] - (me * atoms - atoms)
    relative = jnp.where(relative < 0, relative + everything, relative)
    relative = jnp.where(relative >= everything, relative - everything, relative)
    relative = jnp.minimum(relative, 255)
    rows_ref[...] = relative.astype(jnp.float32).astype(jnp.bfloat16)
    for copy in own:
        copy.wait()

    def prepare(b, carried):
        edge = iota((1, lanes), 1) + b * lanes
        home = edge // slots
        slot = edge - home * slots
        chosen = (iota((atoms, lanes), 0) == home).astype(jnp.bfloat16)
        spread = jnp.dot(rows_ref[...], chosen, preferred_element_type=jnp.float32)
        index = jnp.sum(
            jnp.where(iota((slots, lanes), 0) == slot, spread, 0.0), axis=0, keepdims=True
        ).astype(jnp.int32)
        picked_ref[b] = (iota((extended, lanes), 0) == index).astype(jnp.bfloat16)
        row = pl.ds(pl.multiple_of(b * lanes, lanes), lanes)
        frame_t[b] = lax.dot_general(
            eye(frame_t.shape[1], entries),
            frames_v[row, :],
            ACROSS,
            preferred_element_type=jnp.float32,
        )
        scales = lax.dot_general(
            eye(channels, channels), radial_v[row, :], ACROSS, preferred_element_type=jnp.float32
        ).astype(jnp.bfloat16)
        radial_t[b] = scales.reshape(radial_t.shape[1:])
        return carried

    lax.fori_loop(0, blocks // 6, prepare, 0)

    pairing.wait_recv()
    scatter = []
    for hop in range(1, chips):
        target = lax.rem(my_chip + hop, chips)
        mine = pl.ds(pl.multiple_of(my_core * half + target * part, 16), part)
        there = pl.ds(pl.multiple_of(target * part, 16), part)
        chip_ref[hop - 1] = (
            partial_ref[mine, :].astype(jnp.float32) + paired_ref[there, :].astype(jnp.float32)
        ).astype(jnp.bfloat16)
        scatter.append(
            remote(
                chip_ref.at[hop - 1],
                received_ref.at[hop - 1],
                send_sem.at[hop],
                recv_sem.at[hop],
                (target * 2 + my_core, my_narrow),
            )
        )
        scatter[-1].start()
    lax.fori_loop(blocks // 6, blocks, prepare, 0)
    mine = pl.ds(pl.multiple_of(my_core * half + my_chip * part, 16), part)
    there = pl.ds(pl.multiple_of(my_chip * part, 16), part)
    summed = partial_ref[mine, :].astype(jnp.float32) + paired_ref[there, :].astype(jnp.float32)
    for hop in range(chips - 1):
        scatter[hop].wait_recv()
        summed = summed + received_ref[hop].astype(jnp.float32)
    share_ref[...] = summed.astype(jnp.bfloat16)

    my_place = my_core * chips + my_chip
    keep = pltpu.make_async_copy(share_ref, merged_ref.at[my_narrow, pl.ds(pl.multiple_of(my_place * part, 16), part), :], local_sem)
    keep.start()
    origin = lambda hop: lax.rem(my_narrow + narrow - hop, narrow)

    square = chips == 4
    if square:
        hops = [my_chip + 1 - 2 * lax.rem(my_chip, 2), my_chip + 2 - 4 * (my_chip // 2)]
        far = lax.rem(my_chip + 1, 2) + 2 * (1 - my_chip // 2)
        sources = hops
        owners = [my_chip] + hops + [far]
    else:
        hops = [lax.rem(my_chip + step, chips) for step in range(1, chips)]
        sources = [lax.rem(my_chip + chips - step, chips) for step in range(1, chips)]
        owners = [my_chip] + sources

    def spot(hop, chip, start=0, rows=part):
        row = (my_core * chips + chip) * part + start
        return merged_ref.at[origin(hop), pl.ds(pl.multiple_of(row, 16), rows), :]


    def line_copy(hop):
        return remote(
            share_ref,
            merged_ref.at[my_narrow, pl.ds(pl.multiple_of(my_place * part, 16), part), :],
            line_send.at[hop - 1],
            line_recv.at[hop - 1],
            line[hop - 1],
        )

    def plane_copy(hop, way):
        slot = spot(hop, my_chip)
        at = hop * len(hops) + way
        return remote(
            share_ref if hop == 0 else slot,
            slot,
            plane_send.at[at],
            plane_recv.at[at],
            (hops[way] * 2 + my_core, my_narrow),
        )

    def cross_copy(hop, way):
        slot = spot(hop, hops[way], way * cut, cut if way == 0 else part - cut)
        at = hop * 2 + way
        return remote(
            slot,
            slot,
            cross_send.at[at],
            cross_recv.at[at],
            (hops[1 - way] * 2 + my_core, my_narrow),
        )

    cut = part // 32 * 16

    def crossed(hop, way):
        slot = spot(hop, far, way * cut, cut if way == 0 else part - cut)
        at = hop * 2 + way
        return remote(
            slot,
            slot,
            cross_send.at[at],
            cross_recv.at[at],
            (hops[1 - way] * 2 + my_core, my_narrow),
        )

    def pair_copy(hop, step):
        slot = spot(hop, owners[step])
        at = hop * chips + step
        source = share_ref if hop == 0 and step == 0 else slot
        return remote(source, slot, pair_send.at[at], pair_recv.at[at], partner)

    def forward(hop):
        if hop:
            line_copy(hop).wait_recv()
        for way in range(len(hops)):
            plane_copy(hop, way).start()
        pair_copy(hop, 0).start()

    def relay(hop):
        for way in range(len(hops)):
            plane_copy(hop, way).wait_recv()
            if square:
                cross_copy(hop, way).start()
            pair_copy(hop, way + 1).start()

    def close(hop):
        for way in range(2):
            crossed(hop, way).wait_recv()
        pair_copy(hop, 3).start()

    for hop in range(1, narrow):
        line_copy(hop).start()
    for at in range(EARLY, DEGREES):
        for side in range(2):
            halo_copy(at, side).start()
    forward(0)

    steps = []
    for turn in range(narrow + 2):
        if 0 < turn < narrow:
            steps.append(functools.partial(forward, turn))
        if 0 < turn <= narrow:
            steps.append(functools.partial(relay, turn - 1))
        if square and turn > 1:
            steps.append(functools.partial(close, turn - 2))
    ticks = dict(zip(plan, steps))
    rest = steps[len(plan) :]

    groups, height = radial_t.shape[1:3]
    for at, (degree, base, size) in enumerate(spans()):
        for side in range(2):
            halo_copy(at, side).wait_recv()
        for component in range(base, base + size):
            upright_ref[component] = jnp.transpose(extended_ref[component]).reshape(
                upright_ref.shape[1:]
            )
        first = sum((2 * d + 1) ** 2 for d in range(degree))

        def fetch(b, group, source):
            left = jnp.concatenate(
                [upright_ref[base + q, group] for q in range(size)], axis=0
            )
            got = jnp.dot(left, picked_ref[b], preferred_element_type=jnp.float32)
            for q in range(size):
                source[q, group] = got[q * height : (q + 1) * height].astype(jnp.bfloat16)

        def rotate(b, group, source):
            for lane in range(0, lanes, 128):
                part_of = pl.ds(lane, 128)

                def entry(k):
                    row = frame_t[b, pl.ds(first + k, 1), part_of]
                    row = jnp.broadcast_to(row, (16, 128)).astype(jnp.bfloat16)
                    return jnp.concatenate([row] * (height // 16), axis=0)

                scale = radial_t[b, group, :, part_of]
                xs = [source[q, group, :, part_of] for q in range(size)]
                for p in range(size):
                    value = entry(p * size) * xs[0]
                    for q in range(1, size):
                        value = value + entry(p * size + q) * xs[q]
                    kept_ref[b, base + p, group, :, part_of] = value * scale

        def all_groups(work):
            if size > 5:
                lax.fori_loop(0, groups, lambda group, carried: (work(group), carried)[1], 0)
            else:
                for group in range(groups):
                    work(group)

        buffers = [source_ref, source_b]
        all_groups(lambda group: fetch(0, group, buffers[0]))

        def pair(i, carried):
            for block, step in ticks.items():
                if block // blocks == at:
                    pl.when(i == block % blocks // 2)(step)
            for k in range(2):
                b = 2 * i + k
                following = jnp.minimum(b + 1, blocks - 1)

                def both(group, b=b, following=following, k=k):
                    fetch(following, group, buffers[1 - k])
                    rotate(b, group, buffers[k])

                all_groups(both)
            return carried

        lax.fori_loop(0, blocks // 2, pair, 0)

    for step in rest:
        step()
    for hop in range(narrow):
        for step in range(chips):
            pair_copy(hop, step).wait_recv()
    for hop in range(1, narrow):
        line_copy(hop).wait_send()
    for hop in range(narrow):
        for step in range(chips):
            pair_copy(hop, step).wait_send()
        for way in range(len(hops)):
            plane_copy(hop, way).wait_send()
            if square:
                cross_copy(hop, way).wait_send()
    for copy in scatter + [pairing]:
        copy.wait_send()
    for at in range(DEGREES):
        for side in range(2):
            halo_copy(at, side).wait_send()
    keep.wait()

    offset = 0
    for order, (weight_ref, (rows, columns)) in enumerate(zip(weight_refs, shapes)):
        piece = rows // narrow
        for block in range(columns // 128):
            gathered = jnp.concatenate(
                [merged_ref[m, pl.ds(offset, piece), :] for m in range(narrow)], axis=0
            )
            if order in THREE:
                real = gathered[: rows // 2].astype(jnp.float32)
                imag = gathered[rows // 2 :].astype(jnp.float32)
                gathered = jnp.concatenate([real, real + imag, imag - real], axis=0).astype(
                    jnp.bfloat16
                )
            weight_ref[pl.ds(block * 128, 128), :] = jnp.transpose(gathered)
            offset += piece
    total_ref[...] = jnp.zeros_like(total_ref)
    square = (atoms, atoms)
    diagonal = iota(square, 0) == iota(square, 1)
    count = jnp.sum(
        jnp.where(diagonal, counts_ref[...].astype(jnp.float32), 0.0), axis=1, keepdims=True
    )
    column_ref[...] = jnp.broadcast_to(count, column_ref.shape)

    def mix(b, buffer, beside=lambda: None):
        mix_block(b, kept_ref, weight_refs, buffer, beside)

    def gather(b, buffer):
        sum_block(b, slots, frame_t, buffer, total_ref, column_ref)

    def two(i, carried):
        mix(2 * i + 1, gated_b, lambda: gather(2 * i, gated_ref))
        mix(2 * i + 2, gated_ref, lambda: gather(2 * i + 1, gated_b))
        return carried

    mix(0, gated_ref)
    lax.fori_loop(0, blocks // 2 - 1, two, 0)
    mix(blocks - 1, gated_b, lambda: gather(blocks - 2, gated_ref))
    gather(blocks - 1, gated_b)

    scale = 1.0 / jnp.sqrt(column_ref[...])
    for component in range(COMPONENTS):
        out_ref[component] = total_ref[component] * scale


def mix_block(b, kept_ref, weight_refs, gated_ref, beside):
    channels = gated_ref.shape[0] // COMPONENTS
    lanes = gated_ref.shape[1]
    component_of = lambda degree, order: degree * degree + degree + order
    rows_of = lambda component: pl.ds(component * channels, channels)
    gather = lambda order: jnp.concatenate(
        [
            kept_ref[b, component_of(degree, order)].reshape(channels, lanes)
            for degree in range(abs(order), DEGREES)
        ],
        axis=0,
    )
    central = jnp.dot(weight_refs[0][...], gather(0), preferred_element_type=jnp.float32)
    beside()
    gate = 1.0 / (1.0 + jnp.exp(-central[:channels]))
    for degree in range(DEGREES):
        gated_ref[rows_of(component_of(degree, 0)), :] = (
            central[degree * channels : (degree + 1) * channels] * gate
        ).astype(jnp.bfloat16)
    for order in range(1, DEGREES):
        plus = gather(order)
        minus = gather(-order)
        if order in THREE:
            deep = plus.shape[0]
            full = deep // 256 * 256
            weight = weight_refs[order]
            product = lambda left, right: jnp.dot(left, right, preferred_element_type=jnp.float32)
            fully = lambda at, right: product(
                weight[:, at * deep : at * deep + full], right[:full]
            )
            left_of = lambda at: weight[:, at * deep + full : (at + 1) * deep]
            sums = plus + minus
            both = fully(0, sums)
        for side in range(2):
            if order in THREE:
                other = minus if side == 0 else plus
                term = fully(side + 1, other)
                mixed = both - term if side == 0 else both + term
                if full < deep:
                    tail = -other[full:] if side == 0 else other[full:]
                    mixed = mixed + product(
                        jnp.concatenate([left_of(0), left_of(side + 1)], axis=1),
                        jnp.concatenate([sums[full:], tail], axis=0),
                    )
            else:
                pair = [plus, -minus] if side == 0 else [minus, plus]
                mixed = jnp.dot(
                    weight_refs[order][...],
                    jnp.concatenate(pair, axis=0),
                    preferred_element_type=jnp.float32,
                )
            for column, degree in enumerate(range(order, DEGREES)):
                component = component_of(degree, order if side == 0 else -order)
                gated_ref[rows_of(component), :] = (
                    mixed[column * channels : (column + 1) * channels] * gate
                ).astype(jnp.bfloat16)


def sum_block(b, slots, frame_t, gated_ref, total_ref, column_ref):
    atoms, channels = column_ref.shape
    lanes = gated_ref.shape[1]
    rows_of = lambda component: pl.ds(component * channels, channels)
    edge = iota((1, lanes), 1) + b * lanes
    home = edge // slots
    slot = edge - home * slots
    window = 8
    first = jnp.minimum((b * lanes) // slots, atoms - window)
    position = slot + slots * (home - first) - slots * iota((window, lanes), 0)
    count = column_ref[pl.ds(first, window), :]
    count = jnp.concatenate([count] * (lanes // channels), axis=1)
    live = jnp.where(
        (position >= 0) & (position.astype(jnp.float32) < count) & (position < slots), 1.0, 0.0
    )
    offset = 0
    for degree in range(DEGREES):
        size = 2 * degree + 1
        summed = None
        for q in range(size):
            left = jnp.concatenate(
                [
                    jnp.broadcast_to(frame_t[b, pl.ds(offset + q * size + p, 1), :], live.shape)
                    * live
                    for p in range(size)
                ],
                axis=0,
            ).astype(jnp.bfloat16)
            term = lax.dot_general(
                left,
                gated_ref[rows_of(degree * degree + q), :],
                ACROSS,
                preferred_element_type=jnp.float32,
            )
            summed = term if summed is None else summed + term
        for p in range(size):
            at = degree * degree + p
            total_ref[at, pl.ds(first, window), :] = (
                total_ref[at, pl.ds(first, window), :] + summed[p * window : (p + 1) * window]
            )
        offset += size * size


def run(features, frames, radial, neighbours, counts, coefficients, stacks, lanes, plan):
    shapes = [(int(np.prod(w.shape[1:-1])), w.shape[-1]) for w in stacks]
    wide = lax.axis_size("wide")
    narrow = lax.axis_size("narrow")
    stacks = [flat_rows(w) for w in stacks]
    staged = [(w.shape[0], w.shape[1] // narrow, w.shape[2]) for w in stacks]
    rows = sum(shape[1] * shape[2] // 128 for shape in staged)
    unit = 16 * wide
    rows = -(-rows // unit) * unit
    part = rows // wide
    chips = wide // 2
    components, atoms, channels = features.shape
    edges, entries = frames.shape
    blocks = edges // lanes
    padded = -(-entries // 16) * 16
    groups = 2
    height = channels // groups
    anywhere = pl.BlockSpec(memory_space=pl.ANY)
    vmem = pl.BlockSpec(memory_space=pltpu.VMEM)
    dma = lambda *n: pltpu.SemaphoreType.DMA(n)
    bf16 = lambda *shape: pltpu.VMEM(shape, jnp.bfloat16)
    widest = 2 * DEGREES - 1
    return pl.pallas_call(
        functools.partial(whole_kernel, (wide, narrow, len(stacks)), shapes, plan),
        in_specs=[pl.BlockSpec(memory_space=pltpu.SMEM), vmem, vmem]
        + [anywhere] * (3 + len(stacks)),
        out_specs=vmem,
        out_shape=jax.ShapeDtypeStruct((components, atoms, channels), jnp.float32),
        scratch_shapes=[bf16(*shape) for shape in staged]
        + [bf16(n, k // 2 * 3 if at in THREE else k) for at, (k, n) in enumerate(shapes)]
        + [
            bf16(rows, 128),
            bf16(chips - 1, part, 128),
            bf16(chips * part, 128),
            bf16(chips - 1, part, 128),
            bf16(part, 128),
            bf16(components, 3 * atoms, channels),
            bf16(components, groups, height, 3 * atoms),
            bf16(edges, entries),
            bf16(edges, channels),
            bf16(neighbours.shape[0], atoms),
            bf16(blocks, 3 * atoms, lanes),
            pltpu.VMEM((blocks, padded, lanes), jnp.float32),
            bf16(blocks, groups, height, lanes),
            bf16(widest, groups, height, lanes),
            bf16(widest, groups, height, lanes),
            bf16(blocks, components, groups, height, lanes),
            bf16(narrow, wide * part, 128),
            bf16(components * channels, lanes),
            bf16(components * channels, lanes),
            pltpu.VMEM((components, atoms, channels), jnp.float32),
            pltpu.VMEM((atoms, channels), jnp.float32),
            dma(len(stacks)),
            dma(3),
            dma(2 * DEGREES),
            dma(2 * DEGREES),
            dma(chips),
            dma(chips),
            dma(narrow - 1),
            dma(narrow - 1),
            dma(narrow * (chips - 1)),
            dma(narrow * (chips - 1)),
            dma(narrow * 2),
            dma(narrow * 2),
            dma(narrow * chips),
            dma(narrow * chips),
            pltpu.SemaphoreType.DMA,
        ],
        compiler_params=pltpu.CompilerParams(
            collective_id=0, has_side_effects=True, vmem_limit_bytes=60 * 1024 * 1024
        ),
    )(coefficients, neighbours, counts, features, frames, radial, *stacks)


def body(
    node_features,
    frames,
    radial,
    neighbours,
    counts,
    coefficients,
    w_zero,
    w_one,
    w_two,
    w_three,
    w_four,
):
    atoms, components, channels = node_features.shape
    slots = neighbours.shape[1]
    entries = frames.shape[2]
    edges = atoms * slots
    stacks = (w_zero, w_one, w_two, w_three, w_four)
    lanes = 256
    features = node_features.transpose(1, 0, 2)
    frames = frames.reshape(edges, entries)
    out = run(
        features,
        frames,
        radial.reshape(edges, channels),
        neighbours.T,
        counts.reshape(1, atoms),
        coefficients,
        stacks,
        lanes,
        PLAN,
    )
    return out.transpose(1, 0, 2)


def solution(mesh):
    spread = lambda rest: P(AXES, *([None] * rest))
    in_specs = (
        spread(2),
        spread(2),
        spread(2),
        spread(1),
        spread(0),
        P("wide"),
        P("wide", None, None),
        P("wide", None, None, None),
        P("wide", None, None, None),
        P("wide", None, None, None),
        P("wide", None, None, None),
    )
    return jax.shard_map(body, mesh=mesh, in_specs=in_specs, out_specs=spread(2), check_vma=False)
```
